32 devices in a mesh: expert: 2 (over x), dp: 16 (over z, y, core).
Axes of the slice: x: 2, y: 2, z: 4, core: 2. Of those that a mesh axis runs over, the one named last changes fastest.
Arguments:
- features: bfloat16 [4096, 512], P(('expert', 'dp')), may hold values from -31 to 31
- gradients: bfloat16 [4096, 512], P(('expert', 'dp')), may hold values from -31 to 31
- route_ids: int32 [4096, 2], P(('expert', 'dp')), may hold values from 0 to 7, all different within a row; in each aligned block of 128 rows (0 to 127, 128 to 255, ...) at most 64 rows name the same one
- gate_share: float32 [4096], P(('expert', 'dp')), may hold values from 0.5 to 0.95
- token_mask: int32 [4096], P(('expert', 'dp')), may hold values 0 or 1
- damping: float32 [8, 2, 1], P('expert'), may hold values from 0.5 to 2
Outputs:
- act_inverse: float32 [8, 1, 512, 512], P(None, None, 'dp')
- grad_inverse: float32 [8, 1, 512, 512], P(None, None, 'dp')
The draws below stay inside these ranges and needn't reach their ends.
Inputs may be any that keep to these rules, and one draw needn't show every extreme that they name: `route_ids`: each token names two different experts. Among the 128 tokens of one device no expert is named by more than 64 tokens, a bound that some block reaches.
All inputs are finite; a program needn't handle non-finite values. Where the reference program divides by a largest or mean magnitude, that divisor is 1e-20 or more. No bound on the sum of `token_mask` on one device may be relied on, other than what follows from the above.
Results may differ from the reference program's by a relative error of at most 0.0003.
Values may be sent and summed in bfloat16 or wider, within the bound.
No kernel may reach another device: no remote copies, remote signals or barrier semaphores. Data moves between devices by JAX's collectives and lax.ppermute only.
A program may use at most 64 MiB of HBM per device.

```python
import math
import jax
import jax.numpy as jnp
import numpy as np
from jax import lax

EXPERTS = 8
TOP = 2
BLOCK = 512
NBLK = 1
TOK_DEV = 128
CAP = 64
WIDTH = 512
TOKENS = 4096


def make_rows(key):
    key_normal, key_scale = jax.random.split(key, 2)
    base = jnp.clip(jax.random.normal(key_normal, (TOKENS, WIDTH), jnp.float32), -4.0, 4.0)
    column_scale = jnp.exp(jax.random.uniform(key_scale, (WIDTH,), jnp.float32, math.log(0.3), math.log(3.0)))
    mixed = (base + 0.5 * jnp.roll(base, 1, axis=1)) * column_scale[None, :]
    return mixed.astype(jnp.bfloat16)


def draw_features(key, part):
    return make_rows(jax.random.fold_in(key, 11))


def draw_gradients(key, part):
    return make_rows(jax.random.fold_in(key, 23))


def touch_ends(values, rng, smallest, high):
    shape = values.shape
    spot = [jax.random.randint(jax.random.fold_in(rng, axis), (), 0, shape[axis]) for axis in range(len(shape))]
    values = values.at[tuple(spot)].set(smallest)
    longest = shape.index(max(shape))
    spot[longest] = (spot[longest] + 1) % shape[longest]
    return values.at[tuple(spot)].set(high)


def levels(stream_key, extent, cuts, least, top_value):
    loudness = 1.0
    for position, shards_of in cuts:
        heights = jax.random.uniform(jax.random.fold_in(jax.random.fold_in(stream_key, 6), position), (shards_of,), jnp.float32, least / len(cuts), top_value / len(cuts))
        loudness = loudness * jnp.repeat(jnp.exp(heights), extent[position] // shards_of).reshape((-1,) + (1,) * (len(extent) - 1 - position))
    return loudness


def routed_block(key, own, number, rows, amount, top, reach, skew):
    sequence = jax.random.permutation(key, amount)
    crowded, ordinary = shares(amount, rows * top, reach, skew, True), shares(amount, rows * top, reach, skew, False)
    places = jnp.arange(amount)

    def named(lengths, offset_by):
        used = int((lengths > 0).sum())
        fixed = max(1, used // 4)
        passed = fixed + (places - fixed + offset_by * (used - fixed)) % max(1, amount - fixed)
        return jnp.zeros((amount,), jnp.int32).at[sequence[jnp.where(places < fixed, places, passed)]].set(jnp.asarray(lengths, jnp.int32))

    lengths = jnp.where(number % 4 == 0, named(crowded, number // 4), named(ordinary, number - number // 4 - 1))
    mixed = jax.random.permutation(jax.random.fold_in(own, 3), amount)
    donor, sink = mixed[0:amount // 2 * 2:2], mixed[1:amount // 2 * 2:2]
    slack = jnp.minimum(lengths[donor] - 1, reach - lengths[sink]) // 2
    slack = jnp.where((donor == sequence[0]) | (sink == sequence[0]) | (lengths[sink] == 0), 0, jnp.maximum(slack, 0))
    passed = jax.random.randint(jax.random.fold_in(own, 4), (amount // 2,), 0, 1 << 20) % (slack + 1)
    lengths = lengths.at[donor].add(-passed).at[sink].add(passed)
    items = jnp.searchsorted(jnp.cumsum(lengths), jnp.arange(rows * top), side="right").astype(jnp.int32)
    table = items.reshape(top, rows).T
    table = table[jax.random.permutation(jax.random.fold_in(own, 1), rows)]
    offset_by = jax.random.randint(jax.random.fold_in(own, 2), (rows, 1), 0, top)
    return jnp.take_along_axis(table, (jnp.arange(top)[None, :] + offset_by) % top, axis=1)


def shares(amount, total, most, lean, full):
    weights = [(1 << 20) // math.isqrt(grade ** lean) + 1 for grade in range(1, amount + 1)]
    largest = most if full else min(most, max(-(-total // amount), total * weights[0] // sum(weights)))
    least = 1 if total - largest >= amount - 1 else 0
    given, surplus = [largest] + [least] * (amount - 1), total - largest - least * (amount - 1)
    while surplus > 0:
        candidates = [i for i in range(1, amount) if given[i] < largest] or [i for i in range(1, amount) if given[i] < most]
        pool, budget = sum([weights[i] for i in candidates]), surplus
        for i in candidates:
            extra = min(most - given[i], max(1, budget * weights[i] // pool), surplus)
            given[i] = given[i] + extra
            surplus = surplus - extra
    return np.array(given)


def setup_inputs(seed: int = 0) -> dict:
    arg_keys = jax.random.split(jax.random.key(seed), 7)
    features = draw_features(jax.random.fold_in(arg_keys[6], 71), 0)
    gradients = draw_gradients(jax.random.fold_in(arg_keys[6], 71), 0)
    route_ids_keys = jax.random.split(jax.random.fold_in(arg_keys[2], 1), TOKENS // TOK_DEV)
    route_ids_turns = jax.random.permutation(jax.random.fold_in(arg_keys[2], 3), TOKENS // TOK_DEV)
    route_ids = jax.vmap(lambda own, number: routed_block(jax.random.fold_in(arg_keys[2], 2), own, number, TOK_DEV, EXPERTS, TOP, CAP, 2))(route_ids_keys, route_ids_turns).reshape((TOKENS, TOP))
    gate_share = jnp.clip(0.5 + 0.45 * jax.random.uniform(arg_keys[3], (TOKENS,), jnp.float32) ** levels(arg_keys[3], (TOKENS,), ((0, 32),), -0.2, 0.2), 0.5, 0.95)
    token_mask = touch_ends((jax.random.randint(arg_keys[4], (TOKENS,), 0, 8) < 7).astype(jnp.int32), jax.random.fold_in(arg_keys[4], 1), 0, 1)
    damping = jnp.clip(jnp.exp(math.log(2.0) - 1.3862944 * jax.random.uniform(arg_keys[5], (EXPERTS, 2, NBLK), jnp.float32) ** levels(arg_keys[5], (EXPERTS, 2, NBLK), ((0, 2),), -0.2, 0.2)), 0.5, 2.0)
    return dict(features=features, gradients=gradients, route_ids=route_ids, gate_share=gate_share, token_mask=token_mask, damping=damping)


def newton(iterate, matrix, whole):
    left_product = jnp.einsum("irk,ikc->irc", iterate, matrix, precision=lax.Precision.HIGHEST)
    return 2.0 * iterate - jnp.einsum("irk,ikc->irc", left_product, whole, precision=lax.Precision.HIGHEST)


def reference(features, gradients, route_ids, gate_share, token_mask, damping):
    kept_mask = token_mask.astype(jnp.float32)
    weight_pair = jnp.stack([gate_share, 1.0 - gate_share], axis=1) * kept_mask[:, None]
    rounded = (gradients.astype(jnp.float32)[:, None, :] * weight_pair[:, :, None]).astype(jnp.bfloat16)
    rounded = lax.optimization_barrier(rounded)
    pair_grads = rounded.astype(jnp.float32)
    inputs = features.astype(jnp.float32) * kept_mask[:, None]
    load_inverse = 1.0 / (TOKENS * TOP / EXPERTS)
    experts = jnp.arange(EXPERTS, dtype=jnp.int32)
    damping_flat = damping.reshape(EXPERTS, 2 * NBLK)
    identity = jnp.eye(BLOCK, dtype=jnp.float32)

    def factor_of(packed):
        expert, damping_row = packed
        chosen = (route_ids == expert).astype(jnp.float32)
        member = jnp.sum(chosen, axis=1)
        picked = jnp.sum(pair_grads * chosen[:, :, None], axis=1)
        weighted_inputs = inputs * member[:, None]
        blocks = []
        for source, weighted in ((inputs, weighted_inputs), (picked, picked)):
            for block_index in range(NBLK):
                columns = slice(block_index * BLOCK, (block_index + 1) * BLOCK)
                product = jnp.dot(weighted[:, columns].T, source[:, columns], precision=lax.Precision.HIGHEST, preferred_element_type=jnp.float32)
                blocks.append(product * load_inverse)
        gram_stack = jnp.stack(blocks)
        matrix = gram_stack + damping_row[:, None, None] * identity
        largest_sum = jnp.max(jnp.sum(jnp.abs(matrix), axis=2), axis=1)
        bound_scale = (1.0 / largest_sum)[:, None, None]
        iterate_one = 2.0 * bound_scale * identity - bound_scale * bound_scale * matrix
        iterate_two = newton(iterate_one, matrix, iterate_one)
        return newton(iterate_two, matrix, iterate_two)

    result = lax.map(factor_of, (experts, damping_flat))
    return result[:, :NBLK], result[:, NBLK:]
```

```python
import functools

import jax
import jax.numpy as jnp
from jax import lax
from jax.experimental import pallas as pl
from jax.experimental.pallas import tpu as pltpu
from jax.sharding import PartitionSpec as P

EXPERTS = 8
TOP = 2
BLOCK = 512
NBLK = 1
CAP = 64
WIDTH = 512
FACTORS = 2 * NBLK
MATRICES = EXPERTS * FACTORS
AXES = ("expert", "dp")


def whole(*shape):
    return pl.BlockSpec(memory_space=pltpu.VMEM)


def pack_kernel(features, gradients, routes, share, mask, out):
    tokens = features.shape[0]
    first, second = routes[0:1, :], routes[1:2, :]
    kept = mask[...] > 0
    expert = lax.broadcasted_iota(jnp.int32, (EXPERTS, tokens), 0)
    is_first, is_second = expert == first, expert == second
    member = jnp.where(is_first | is_second, 1.0, 0.0).astype(jnp.bfloat16)
    earlier = lax.broadcasted_iota(jnp.int32, (tokens, tokens), 0) < lax.broadcasted_iota(
        jnp.int32, (tokens, tokens), 1
    )
    position = jnp.dot(
        member,
        jnp.where(earlier, 1.0, 0.0).astype(jnp.bfloat16),
        preferred_element_type=jnp.float32,
    )

    def target(chosen, ids):
        place = jnp.sum(jnp.where(chosen, position, 0.0), axis=0, keepdims=True)
        return ids * CAP + place.astype(jnp.int32)

    slot = lax.broadcasted_iota(jnp.int32, (EXPERTS * CAP, tokens), 0)
    pick_first = slot == target(is_first, first)
    pick_second = slot == target(is_second, second)
    pick = jnp.where((pick_first | pick_second) & kept, 1.0, 0.0).astype(jnp.bfloat16)
    rows = jnp.dot(pick, features[...], preferred_element_type=jnp.float32)
    out[:, 0] = rows.astype(jnp.bfloat16).reshape(EXPERTS, CAP, WIDTH)

    kept_mask = mask[...].astype(jnp.float32)
    wide = gradients[...].astype(jnp.float32)

    def weighted(weight):
        column = jnp.transpose(jnp.broadcast_to(weight * kept_mask, (tokens, tokens)))
        column = jnp.concatenate([column] * (WIDTH // tokens), axis=1)
        return (wide * column).astype(jnp.bfloat16)

    pairs = jnp.concatenate([weighted(share[...]), weighted(1.0 - share[...])], axis=0)
    picks = jnp.concatenate(
        [
            jnp.where(pick_first, 1.0, 0.0).astype(jnp.bfloat16),
            jnp.where(pick_second, 1.0, 0.0).astype(jnp.bfloat16),
        ],
        axis=1,
    )
    rows = jnp.dot(picks, pairs, preferred_element_type=jnp.float32)
    out[:, 1] = rows.astype(jnp.bfloat16).reshape(EXPERTS, CAP, WIDTH)


def gram_kernel(rows, out):
    out[...] = lax.dot_general(
        rows[...], rows[...], (((0,), (0,)), ((), ())), preferred_element_type=jnp.float32
    )


def split(value):
    high = value.astype(jnp.bfloat16)
    return high, (value - high.astype(jnp.float32)).astype(jnp.bfloat16)


def product(left, right):
    (left_high, left_low), (right_high, right_low) = left, right

    def dot(a, b):
        return jnp.dot(a, b, preferred_element_type=jnp.float32)

    return dot(left_high, right_high) + (dot(left_high, right_low) + dot(left_low, right_high))


def newton_kernel(load_inverse, owners, shards, damping, mine, other, out):
    core = lax.rem(lax.axis_index("dp"), owners)
    place = lax.broadcasted_iota(jnp.int32, (BLOCK, BLOCK), 0)
    identity = jnp.where(place == lax.broadcasted_iota(jnp.int32, (BLOCK, BLOCK), 1), 1.0, 0.0)
    matrix = (mine[...] + other[...]) * load_inverse + damping[0] * identity
    bound = jnp.max(jnp.sum(jnp.abs(matrix), axis=0, keepdims=True), axis=1, keepdims=True)
    scale = 1.0 / bound
    error = identity - scale * matrix
    parts = split(error)
    square = split(product(parts, parts))
    start = (identity + error).reshape(shards, owners, BLOCK // (shards * owners), BLOCK)
    rows = start[:, 0]
    for turn in range(1, owners):
        rows = jnp.where(core == turn, start[:, turn], rows)
    rows = rows.reshape(BLOCK // owners, BLOCK)
    rows = rows + product(split(rows), square)
    last = rows + product(split(product(split(rows), square)), square)
    last = scale * last
    for copy in range(out.shape[0]):
        out[copy] = last


def owned(features, gradients, route_ids, gate_share, token_mask, damping):
    tokens = features.shape[0]
    experts_axis, shards = lax.axis_size("expert"), lax.axis_size("dp")
    devices = experts_axis * shards
    owners = devices // MATRICES
    load_inverse = 1.0 / (tokens * devices * TOP / EXPERTS)
    spec = whole()
    packed = pl.pallas_call(
        pack_kernel,
        out_shape=jax.ShapeDtypeStruct((EXPERTS, FACTORS, CAP, WIDTH), jnp.bfloat16),
        in_specs=[spec] * 5,
        out_specs=spec,
        name="pack",
    )(
        features,
        gradients,
        route_ids.T,
        gate_share.reshape(1, tokens),
        token_mask.reshape(1, tokens),
    )
    packed = packed.reshape(MATRICES * CAP, WIDTH)
    received = lax.all_to_all(packed, AXES, split_axis=0, concat_axis=0, tiled=True)
    mine = pl.pallas_call(
        gram_kernel,
        out_shape=jax.ShapeDtypeStruct((BLOCK, BLOCK), jnp.float32),
        in_specs=[spec],
        out_specs=spec,
        name="gram",
    )(received)
    other = lax.ppermute(mine, "dp", [(i, i ^ 1) for i in range(shards)])
    own_damping = lax.dynamic_slice_in_dim(
        damping.reshape(-1), lax.axis_index("dp") // owners, 1, 0
    )
    rows = pl.pallas_call(
        functools.partial(newton_kernel, load_inverse, owners, shards),
        out_shape=jax.ShapeDtypeStruct((experts_axis, BLOCK // owners, BLOCK), jnp.float32),
        in_specs=[pl.BlockSpec(memory_space=pltpu.SMEM), spec, spec],
        out_specs=spec,
        name="newton",
    )(own_damping, mine, other)
    rows = rows.reshape(experts_axis * BLOCK // owners, BLOCK)
    gathered = lax.all_to_all(rows, AXES, split_axis=0, concat_axis=0, tiled=True)
    gathered = gathered.reshape(EXPERTS, FACTORS, NBLK, BLOCK // shards, BLOCK)
    return gathered[:, 0], gathered[:, 1]


def slot_table(route_ids, capacity):
    pair_experts = route_ids.reshape(-1)
    onehot = (pair_experts[:, None] == jnp.arange(EXPERTS, dtype=jnp.int32)[None, :]).astype(
        jnp.int32
    )
    running = jnp.cumsum(onehot, axis=0)
    position = jnp.sum(onehot * running, axis=1) - 1
    target = pair_experts * capacity + position
    sources = jnp.arange(1, pair_experts.shape[0] + 1, dtype=jnp.int32)
    return jnp.zeros((EXPERTS * capacity,), jnp.int32).at[target].set(sources)


def newton_rows(rows_now, matrix, whole_now):
    left_product = jnp.einsum("eirk,eikc->eirc", rows_now, matrix, precision=lax.Precision.HIGHEST)
    return 2.0 * rows_now - jnp.einsum(
        "eirk,eikc->eirc", left_product, whole_now, precision=lax.Precision.HIGHEST
    )


def first_iterate(matrix, identity, inverse_bound):
    bound_scale = inverse_bound[:, :, None, None]
    return 2.0 * bound_scale * identity - bound_scale * bound_scale * matrix


def shared(features, gradients, route_ids, gate_share, token_mask, damping):
    tokens_here = features.shape[0]
    capacity = CAP
    blocks = 2 * NBLK
    kept_mask = token_mask.astype(jnp.float32)
    weight_pair = jnp.stack([gate_share, 1.0 - gate_share], axis=1) * kept_mask[:, None]
    kept_rows = features * token_mask.astype(jnp.bfloat16)[:, None]
    pair_grads = (gradients[:, None, :].astype(jnp.float32) * weight_pair[:, :, None]).astype(
        jnp.bfloat16
    )
    repeated = jnp.broadcast_to(kept_rows[:, None, :], pair_grads.shape)
    pair_rows = jnp.concatenate([repeated, pair_grads], axis=2).reshape(
        tokens_here * TOP, 2 * WIDTH
    )
    padded = jnp.concatenate([jnp.zeros((1, 2 * WIDTH), jnp.bfloat16), pair_rows], axis=0)
    buffer = jnp.take(padded, slot_table(route_ids, capacity), axis=0).reshape(
        EXPERTS, capacity, blocks, BLOCK
    )
    load_inverse = 1.0 / (
        tokens_here * lax.axis_size("expert") * lax.axis_size("dp") * TOP / EXPERTS
    )
    received = lax.all_to_all(buffer, "expert", split_axis=0, concat_axis=1, tiled=True)
    gram_blocks = (
        jnp.einsum("erib,eric->eibc", received, received, preferred_element_type=jnp.float32)
        * load_inverse
    )
    damping_flat = damping.reshape(damping.shape[0], blocks)[:, :, None, None]
    rows_share = BLOCK // lax.axis_size("dp")
    row_start = lax.axis_index("dp") * rows_share
    identity = jnp.eye(BLOCK, dtype=jnp.float32)
    summed = lax.psum(gram_blocks, "dp")
    matrix = summed + damping_flat * identity
    largest_sum = jnp.max(jnp.sum(jnp.abs(matrix), axis=3), axis=2)
    inverse_bound = 1.0 / largest_sum
    iterate_one = first_iterate(matrix, identity, inverse_bound)
    iterate_two = newton_rows(iterate_one, matrix, iterate_one)
    second_rows = lax.dynamic_slice_in_dim(iterate_two, row_start, rows_share, 2)
    third_rows = newton_rows(second_rows, matrix, iterate_two)
    act_rows = third_rows[:, :NBLK]
    grad_rows = third_rows[:, NBLK:]
    return (
        lax.all_gather(act_rows, "expert", axis=0, tiled=True),
        lax.all_gather(grad_rows, "expert", axis=0, tiled=True),
    )


def solution(mesh):
    placed = (
        P(("expert", "dp"), None),
        P(("expert", "dp"), None),
        P(("expert", "dp"), None),
        P(("expert", "dp")),
        P(("expert", "dp")),
        P("expert", None, None),
    )
    paired = mesh.shape["expert"] * mesh.shape["dp"] == 2 * MATRICES
    return jax.shard_map(
        owned if paired else shared,
        mesh=mesh,
        in_specs=placed,
        out_specs=(P(None, None, "dp", None), P(None, None, "dp", None)),
        check_vma=False,
    )
```

```python
import functools

import jax
import jax.numpy as jnp
from jax import lax
from jax.experimental import pallas as pl
from jax.experimental.pallas import tpu as pltpu
from jax.sharding import PartitionSpec as P

EXPERTS = 8
TOP = 2
BLOCK = 512
NBLK = 1
CAP = 64
WIDTH = 512
FACTORS = 2 * NBLK
MATRICES = EXPERTS * FACTORS
LANES = 128
VMEM_GRANT = 16 * 2**20
SENT_SCALE = 2.0**14
AXES = ("expert", "dp")


def whole(*shape):
    return pl.BlockSpec(memory_space=pltpu.VMEM)


def pack_kernel(features, gradients, routes, share, mask, out):
    tokens = features.shape[0]
    first, second = routes[0:1, :], routes[1:2, :]
    kept = mask[...] > 0
    expert = lax.broadcasted_iota(jnp.int32, (EXPERTS, tokens), 0)
    is_first, is_second = expert == first, expert == second
    member = jnp.where(is_first | is_second, 1.0, 0.0).astype(jnp.bfloat16)
    earlier = lax.broadcasted_iota(jnp.int32, (tokens, tokens), 0) < lax.broadcasted_iota(
        jnp.int32, (tokens, tokens), 1
    )
    position = jnp.dot(
        member,
        jnp.where(earlier, 1.0, 0.0).astype(jnp.bfloat16),
        preferred_element_type=jnp.float32,
    )

    def target(chosen, ids):
        place = jnp.sum(jnp.where(chosen, position, 0.0), axis=0, keepdims=True)
        return ids * CAP + place.astype(jnp.int32)

    slot = lax.broadcasted_iota(jnp.int32, (EXPERTS * CAP, tokens), 0)
    pick_first = slot == target(is_first, first)
    pick_second = slot == target(is_second, second)
    pick = jnp.where((pick_first | pick_second) & kept, 1.0, 0.0).astype(jnp.bfloat16)
    rows = jnp.dot(pick, features[...], preferred_element_type=jnp.float32)
    out[:, 0] = rows.astype(jnp.bfloat16).reshape(EXPERTS, CAP, WIDTH)

    kept_mask = mask[...].astype(jnp.float32)
    wide = gradients[...].astype(jnp.float32)

    def weighted(weight):
        column = jnp.transpose(jnp.broadcast_to(weight * kept_mask, (tokens, tokens)))
        column = jnp.concatenate([column] * (WIDTH // tokens), axis=1)
        return (wide * column).astype(jnp.bfloat16)

    pairs = jnp.concatenate([weighted(share[...]), weighted(1.0 - share[...])], axis=0)
    picks = jnp.concatenate(
        [
            jnp.where(pick_first, 1.0, 0.0).astype(jnp.bfloat16),
            jnp.where(pick_second, 1.0, 0.0).astype(jnp.bfloat16),
        ],
        axis=1,
    )
    rows = jnp.dot(picks, pairs, preferred_element_type=jnp.float32)
    out[:, 1] = rows.astype(jnp.bfloat16).reshape(EXPERTS, CAP, WIDTH)


def gram_kernel(rows, out):
    out[...] = lax.dot_general(
        rows[...], rows[...], (((0,), (0,)), ((), ())), preferred_element_type=jnp.float32
    )


def split(value):
    high = value.astype(jnp.bfloat16)
    return high, (value - high.astype(jnp.float32)).astype(jnp.bfloat16)


def product(left, right):
    (left_high, left_low), (right_high, right_low) = left, right

    def dot(a, b):
        return jnp.dot(a, b, preferred_element_type=jnp.float32)

    return dot(left_high, right_high) + (dot(left_high, right_low) + dot(left_low, right_high))


def newton_kernel(load_inverse, owners, shards, damping, mine, other, out):
    shard = lax.axis_index("dp")
    core, own = lax.rem(shard, owners), shard // owners
    place = lax.broadcasted_iota(jnp.int32, (BLOCK, BLOCK), 0)
    identity = jnp.where(place == lax.broadcasted_iota(jnp.int32, (BLOCK, BLOCK), 1), 1.0, 0.0)
    matrix = (mine[...] + other[...]) * load_inverse + damping[lax.rem(own, FACTORS), own // FACTORS] * identity
    bound = jnp.max(jnp.sum(jnp.abs(matrix), axis=0, keepdims=True), axis=1, keepdims=True)
    scale = 1.0 / bound
    error = identity - scale * matrix
    parts = split(error)
    square = split(product(parts, parts))
    start = (identity + error).reshape(shards, owners, BLOCK // (shards * owners), BLOCK)
    rows = start[:, 0]
    for turn in range(1, owners):
        rows = jnp.where(core == turn, start[:, turn], rows)
    rows = rows.reshape(BLOCK // owners, BLOCK)
    rows = rows + product(split(rows), square)
    last = rows + product(split(product(split(rows), square)), square)
    last = (scale * SENT_SCALE) * last
    encode(core, shards, owners, last, out)


def encode(core, shards, owners, rows, out):
    share = BLOCK // (shards * owners)
    out[...] = rows
    row = lax.broadcasted_iota(jnp.int32, (share, LANES), 0)
    lane = lax.broadcasted_iota(jnp.int32, (share, LANES), 1)
    for shard in range(shards):
        first = shard * share * owners
        start = first // LANES * LANES
        tile = rows[shard * share : (shard + 1) * share, start : start + LANES]
        column = lane - (first - start + core * share)
        diagonal = jnp.sum(jnp.where(column == row, tile, 0.0), axis=1, keepdims=True)
        high = diagonal.astype(jnp.bfloat16).astype(jnp.float32)
        low = diagonal - high
        tile = jnp.where(column == row, high, tile)
        tile = jnp.where((column == row - 1) & (row > 0), low, tile)
        tile = jnp.where((column == 0) & (row == 2), low[0:1, :], tile)
        out[shard * share : (shard + 1) * share, start : start + LANES] = tile


def decode_kernel(owners, share, rows, act, grad):
    shard = lax.axis_index("dp")
    per_factor = owners * share
    first = shard * per_factor
    start = pl.multiple_of(first // LANES * LANES, LANES)
    sent = rows[...] * (1.0 / SENT_SCALE)
    for out, factor in ((act, 0), (grad, 1)):
        out[:, 0] = sent.reshape(EXPERTS, FACTORS, per_factor, BLOCK)[:, factor]
    total = rows.shape[0]
    tile = rows[:, pl.ds(start, LANES)] * (1.0 / SENT_SCALE)
    place = lax.broadcasted_iota(jnp.int32, (total, LANES), 0)
    row = lax.rem(place, share)
    core = lax.rem(place // share, owners)
    column = lax.broadcasted_iota(jnp.int32, (total, LANES), 1) - (first - start + core * share)

    def moved(down, right):
        value = tile
        if down:
            value = pltpu.roll(value, down % total, 0)
        if right:
            value = pltpu.roll(value, right % LANES, 1)
        return value

    fixed = jnp.where(column == row, tile + jnp.where(row > 0, moved(0, 1), moved(-2, 0)), tile)
    fixed = jnp.where((column == row - 1) & (row > 0), moved(1, -1), fixed)
    fixed = jnp.where((column == 0) & (row == 2), moved(2, -2), fixed)
    fixed = fixed.reshape(EXPERTS, FACTORS, per_factor, LANES)
    for out, factor in ((act, 0), (grad, 1)):
        out[:, 0, :, pl.ds(start, LANES)] = fixed[:, factor]


def owned(features, gradients, route_ids, gate_share, token_mask, damping):
    tokens = features.shape[0]
    experts_axis, shards = lax.axis_size("expert"), lax.axis_size("dp")
    devices = experts_axis * shards
    owners = devices // MATRICES
    load_inverse = 1.0 / (tokens * devices * TOP / EXPERTS)
    spec = whole()
    packed = pl.pallas_call(
        pack_kernel,
        out_shape=pltpu.VMEM((EXPERTS, FACTORS, CAP, WIDTH), jnp.bfloat16),
        in_specs=[spec] * 5,
        out_specs=spec,
        compiler_params=pltpu.CompilerParams(vmem_limit_bytes=VMEM_GRANT),
        name="pack",
    )(
        features,
        gradients,
        route_ids.T,
        gate_share.reshape(1, tokens),
        token_mask.reshape(1, tokens),
    )
    packed = packed.reshape(MATRICES * CAP, WIDTH)
    received = lax.all_to_all(packed, AXES, split_axis=0, concat_axis=0, tiled=True)
    mine = pl.pallas_call(
        gram_kernel,
        out_shape=pltpu.VMEM((BLOCK, BLOCK), jnp.float32),
        in_specs=[spec],
        out_specs=spec,
        compiler_params=pltpu.CompilerParams(vmem_limit_bytes=VMEM_GRANT),
        name="gram",
    )(received)
    other = lax.ppermute(mine, "dp", [(i, i ^ 1) for i in range(shards)])
    rows = pl.pallas_call(
        functools.partial(newton_kernel, load_inverse, owners, shards),
        out_shape=pltpu.VMEM((BLOCK // owners, BLOCK), jnp.float32),
        in_specs=[pl.BlockSpec(memory_space=pltpu.SMEM), spec, spec],
        out_specs=spec,
        compiler_params=pltpu.CompilerParams(vmem_limit_bytes=VMEM_GRANT),
        name="newton",
    )(damping.reshape(-1, FACTORS).T, mine, other)
    sent = jnp.concatenate([rows.astype(jnp.float16)] * experts_axis, axis=0)
    gathered = lax.all_to_all(sent, AXES, split_axis=0, concat_axis=0, tiled=True)
    share = BLOCK // (shards * owners)
    result = jax.ShapeDtypeStruct((EXPERTS, NBLK, BLOCK // shards, BLOCK), jnp.float32)
    return pl.pallas_call(
        functools.partial(decode_kernel, owners, share),
        out_shape=(result, result),
        in_specs=[spec],
        out_specs=(spec, spec),
        compiler_params=pltpu.CompilerParams(vmem_limit_bytes=VMEM_GRANT),
        name="decode",
    )(gathered.astype(jnp.float32))


def slot_table(route_ids, capacity):
    pair_experts = route_ids.reshape(-1)
    onehot = (pair_experts[:, None] == jnp.arange(EXPERTS, dtype=jnp.int32)[None, :]).astype(
        jnp.int32
    )
    running = jnp.cumsum(onehot, axis=0)
    position = jnp.sum(onehot * running, axis=1) - 1
    target = pair_experts * capacity + position
    sources = jnp.arange(1, pair_experts.shape[0] + 1, dtype=jnp.int32)
    return jnp.zeros((EXPERTS * capacity,), jnp.int32).at[target].set(sources)


def newton_rows(rows_now, matrix, whole_now):
    left_product = jnp.einsum("eirk,eikc->eirc", rows_now, matrix, precision=lax.Precision.HIGHEST)
    return 2.0 * rows_now - jnp.einsum(
        "eirk,eikc->eirc", left_product, whole_now, precision=lax.Precision.HIGHEST
    )


def first_iterate(matrix, identity, inverse_bound):
    bound_scale = inverse_bound[:, :, None, None]
    return 2.0 * bound_scale * identity - bound_scale * bound_scale * matrix


def shared(features, gradients, route_ids, gate_share, token_mask, damping):
    tokens_here = features.shape[0]
    capacity = CAP
    blocks = 2 * NBLK
    kept_mask = token_mask.astype(jnp.float32)
    weight_pair = jnp.stack([gate_share, 1.0 - gate_share], axis=1) * kept_mask[:, None]
    kept_rows = features * token_mask.astype(jnp.bfloat16)[:, None]
    pair_grads = (gradients[:, None, :].astype(jnp.float32) * weight_pair[:, :, None]).astype(
        jnp.bfloat16
    )
    repeated = jnp.broadcast_to(kept_rows[:, None, :], pair_grads.shape)
    pair_rows = jnp.concatenate([repeated, pair_grads], axis=2).reshape(
        tokens_here * TOP, 2 * WIDTH
    )
    padded = jnp.concatenate([jnp.zeros((1, 2 * WIDTH), jnp.bfloat16), pair_rows], axis=0)
    buffer = jnp.take(padded, slot_table(route_ids, capacity), axis=0).reshape(
        EXPERTS, capacity, blocks, BLOCK
    )
    load_inverse = 1.0 / (
        tokens_here * lax.axis_size("expert") * lax.axis_size("dp") * TOP / EXPERTS
    )
    received = lax.all_to_all(buffer, "expert", split_axis=0, concat_axis=1, tiled=True)
    gram_blocks = (
        jnp.einsum("erib,eric->eibc", received, received, preferred_element_type=jnp.float32)
        * load_inverse
    )
    damping_flat = damping.reshape(damping.shape[0], blocks)[:, :, None, None]
    rows_share = BLOCK // lax.axis_size("dp")
    row_start = lax.axis_index("dp") * rows_share
    identity = jnp.eye(BLOCK, dtype=jnp.float32)
    summed = lax.psum(gram_blocks, "dp")
    matrix = summed + damping_flat * identity
    largest_sum = jnp.max(jnp.sum(jnp.abs(matrix), axis=3), axis=2)
    inverse_bound = 1.0 / largest_sum
    iterate_one = first_iterate(matrix, identity, inverse_bound)
    iterate_two = newton_rows(iterate_one, matrix, iterate_one)
    second_rows = lax.dynamic_slice_in_dim(iterate_two, row_start, rows_share, 2)
    third_rows = newton_rows(second_rows, matrix, iterate_two)
    act_rows = third_rows[:, :NBLK]
    grad_rows = third_rows[:, NBLK:]
    return (
        lax.all_gather(act_rows, "expert", axis=0, tiled=True),
        lax.all_gather(grad_rows, "expert", axis=0, tiled=True),
    )


def solution(mesh):
    placed = (
        P(("expert", "dp"), None),
        P(("expert", "dp"), None),
        P(("expert", "dp"), None),
        P(("expert", "dp")),
        P(("expert", "dp")),
        P("expert", None, None),
    )
    paired = mesh.shape["expert"] * mesh.shape["dp"] == 2 * MATRICES
    return jax.shard_map(
        owned if paired else shared,
        mesh=mesh,
        in_specs=placed,
        out_specs=(P(None, None, "dp", None), P(None, None, "dp", None)),
        check_vma=False,
    )
```

```python
import functools

import jax
import jax.numpy as jnp
from jax import lax
from jax.experimental import pallas as pl
from jax.experimental.pallas import tpu as pltpu
from jax.sharding import PartitionSpec as P

EXPERTS = 8
TOP = 2
BLOCK = 512
NBLK = 1
CAP = 64
WIDTH = 512
FACTORS = 2 * NBLK
MATRICES = EXPERTS * FACTORS
OWNERS = 2
LANES = 128
VMEM_GRANT = 16 * 2**20
COLLECT_GRANT = 60 * 2**20
SENT_SCALE = 2.0**14
AXES = ("expert", "dp")


def whole(*shape):
    return pl.BlockSpec(memory_space=pltpu.VMEM)


META = 8


def chip_of(expert_shard, shard, shards):
    chips = shards // FACTORS // OWNERS
    return expert_shard * chips + lax.rem(shard, chips * OWNERS) // OWNERS


def collect_kernel(features, gradients, routes, share, mask, own, sent, ids, weight, kept, sems):
    tokens = features.shape[0]
    lower = lax.axis_index("dp") < lax.axis_size("dp") // FACTORS
    small = [
        pltpu.make_async_copy(routes, ids, sems.at[2]),
        pltpu.make_async_copy(share, weight, sems.at[3]),
        pltpu.make_async_copy(mask, kept, sems.at[4]),
    ]
    for copy in small:
        copy.start()

    def tokens_in(source, target, sem):
        return pltpu.make_async_copy(source, target.at[0:tokens], sems.at[sem])

    @pl.when(lower)
    def _():
        tokens_in(gradients, sent, 0).start()
        tokens_in(features, own, 1).start()

    @pl.when(jnp.logical_not(lower))
    def _():
        tokens_in(features, sent, 0).start()
        tokens_in(gradients, own, 1).start()

    for copy in small:
        copy.wait()
    high = weight[...].astype(jnp.bfloat16).astype(jnp.float32)
    rest = weight[...] - high
    middle = rest.astype(jnp.bfloat16).astype(jnp.float32)
    low = rest - middle
    first = jnp.concatenate(
        [
            ids[0:1, :].astype(jnp.float32),
            ids[1:2, :].astype(jnp.float32),
            kept[...].astype(jnp.float32),
            high,
        ],
        axis=1,
    )
    second = jnp.concatenate([middle, low, jnp.zeros_like(low), jnp.zeros_like(low)], axis=1)
    row = lax.broadcasted_iota(jnp.int32, (META, WIDTH), 0)
    meta = jnp.where(row == 0, first, jnp.where(row == 1, second, 0.0)).astype(jnp.bfloat16)
    own[tokens : tokens + META, :] = meta
    sent[tokens : tokens + META, :] = meta
    tokens_in(features, sent, 0).wait()
    tokens_in(features, own, 1).wait()


def pack_kernel(packages, *refs):
    inputs, outputs = refs[:packages], refs[packages:]
    tokens = inputs[0].shape[0] - META
    shard, shards = lax.axis_index("dp"), lax.axis_size("dp")
    lower = shard < shards // FACTORS
    chip = chip_of(lax.axis_index("expert"), shard, shards)
    expert = lax.broadcasted_iota(jnp.int32, (EXPERTS, tokens), 0)
    earlier = lax.broadcasted_iota(jnp.int32, (tokens, tokens), 0) < lax.broadcasted_iota(
        jnp.int32, (tokens, tokens), 1
    )
    earlier = jnp.where(earlier, 1.0, 0.0).astype(jnp.bfloat16)
    slot = lax.broadcasted_iota(jnp.int32, (EXPERTS * CAP, tokens), 0)
    for place, package in enumerate(inputs):
        meta = package[tokens : tokens + META, :].astype(jnp.float32)

        def part(row, index):
            return meta[row : row + 1, index * tokens : (index + 1) * tokens]

        first = part(0, 0).astype(jnp.int32) ^ chip
        second = part(0, 1).astype(jnp.int32) ^ chip
        kept = part(0, 2)
        share = (part(0, 3) + part(1, 0)) + part(1, 1)
        is_first, is_second = expert == first, expert == second
        member = jnp.where(is_first | is_second, 1.0, 0.0).astype(jnp.bfloat16)
        position = jnp.dot(member, earlier, preferred_element_type=jnp.float32)
        wide = package[0:tokens, :].astype(jnp.float32)

        def picked(chosen, named):
            spot = jnp.sum(jnp.where(chosen, position, 0.0), axis=0, keepdims=True)
            hit = slot == named * CAP + spot.astype(jnp.int32)
            return jnp.where(hit, 1.0, 0.0).astype(jnp.bfloat16)

        def weighted(weight):
            weight = jnp.where(lower, kept, weight * kept)
            column = jnp.transpose(jnp.broadcast_to(weight, (tokens, tokens)))
            column = jnp.concatenate([column] * (WIDTH // tokens), axis=1)
            return (wide * column).astype(jnp.bfloat16)

        picks = jnp.concatenate([picked(is_first, first), picked(is_second, second)], axis=1)
        pairs = jnp.concatenate([weighted(share), weighted(1.0 - share)], axis=0)
        rows = jnp.dot(picks, pairs, preferred_element_type=jnp.float32)
        rows = rows.astype(jnp.bfloat16)
        for step, out in enumerate(outputs):
            out[place * CAP : (place + 1) * CAP, :] = rows[step * CAP : (step + 1) * CAP]


def gram_kernel(*refs):
    rows = jnp.concatenate([ref[...] for ref in refs[:-1]], axis=0)
    refs[-1][...] = lax.dot_general(
        rows, rows, (((0,), (0,)), ((), ())), preferred_element_type=jnp.float32
    )


def split(value):
    high = value.astype(jnp.bfloat16)
    return high, (value - high.astype(jnp.float32)).astype(jnp.bfloat16)


def product(left, right):
    (left_high, left_low), (right_high, right_low) = left, right

    def dot(a, b):
        return jnp.dot(a, b, preferred_element_type=jnp.float32)

    return dot(left_high, right_high) + (dot(left_high, right_low) + dot(left_low, right_high))


def newton_kernel(load_inverse, owners, shards, damping, mine, other, out):
    shard = lax.axis_index("dp")
    core = lax.rem(shard, owners)
    factor = shard // (shards // FACTORS)
    expert = lax.rem(shard, shards // FACTORS) // owners
    place = lax.broadcasted_iota(jnp.int32, (BLOCK, BLOCK), 0)
    identity = jnp.where(place == lax.broadcasted_iota(jnp.int32, (BLOCK, BLOCK), 1), 1.0, 0.0)
    matrix = (mine[...] + other[...]) * load_inverse + damping[factor, expert] * identity
    bound = jnp.max(jnp.sum(jnp.abs(matrix), axis=0, keepdims=True), axis=1, keepdims=True)
    scale = 1.0 / bound
    error = identity - scale * matrix
    parts = split(error)
    square = split(product(parts, parts))
    start = (identity + error).reshape(shards // owners, owners, BLOCK // shards, BLOCK)
    rows = start[:, 0]
    for turn in range(1, owners):
        rows = jnp.where(core == turn, start[:, turn], rows)
    rows = rows.reshape(BLOCK // owners, BLOCK)
    rows = rows + product(split(rows), square)
    last = rows + product(split(product(split(rows), square)), square)
    last = (scale * SENT_SCALE) * last
    encode(core, shards, owners, last, out)


def encode(core, shards, owners, rows, out):
    share = BLOCK // shards
    out[...] = rows
    row = lax.broadcasted_iota(jnp.int32, (share, LANES), 0)
    lane = lax.broadcasted_iota(jnp.int32, (share, LANES), 1)
    for turn in range(shards // owners):
        first = turn * owners * share
        start = first // LANES * LANES
        tile = rows[turn * share : (turn + 1) * share, start : start + LANES]
        column = lane - (first - start + core * share)
        diagonal = jnp.sum(jnp.where(column == row, tile, 0.0), axis=1, keepdims=True)
        high = diagonal.astype(jnp.bfloat16).astype(jnp.float32)
        low = diagonal - high
        tile = jnp.where(column == row, high, tile)
        tile = jnp.where((column == row - 1) & (row > 0), low, tile)
        tile = jnp.where((column == 0) & (row == 2), low[0:1, :], tile)
        out[turn * share : (turn + 1) * share, start : start + LANES] = tile


def decode_kernel(rows, act, grad):
    groups, share = lax.axis_size("expert"), act.shape[2]
    first = lax.axis_index("dp") * share
    start = pl.multiple_of(first // LANES * LANES, LANES)

    def by_factor(value):
        value = value.reshape(groups, FACTORS, EXPERTS // groups, share, value.shape[-1])
        return (
            (out, value[:, factor].reshape(EXPERTS, share, value.shape[-1]))
            for out, factor in ((act, 0), (grad, 1))
        )

    for out, value in by_factor(rows[...] * (1.0 / SENT_SCALE)):
        out[:, 0] = value
    total = rows.shape[0]
    tile = rows[:, pl.ds(start, LANES)] * (1.0 / SENT_SCALE)
    row = lax.rem(lax.broadcasted_iota(jnp.int32, (total, LANES), 0), share)
    column = lax.broadcasted_iota(jnp.int32, (total, LANES), 1) - (first - start)

    def moved(down, right):
        value = tile
        if down:
            value = pltpu.roll(value, down % total, 0)
        if right:
            value = pltpu.roll(value, right % LANES, 1)
        return value

    fixed = jnp.where(column == row, tile + jnp.where(row > 0, moved(0, 1), moved(-2, 0)), tile)
    fixed = jnp.where((column == row - 1) & (row > 0), moved(1, -1), fixed)
    fixed = jnp.where((column == 0) & (row == 2), moved(2, -2), fixed)
    for out, value in by_factor(fixed):
        out[:, 0, :, pl.ds(start, LANES)] = value


def owned(features, gradients, route_ids, gate_share, token_mask, damping):
    tokens = features.shape[0]
    experts_axis, shards = lax.axis_size("expert"), lax.axis_size("dp")
    devices = experts_axis * shards
    owners = devices // MATRICES
    load_inverse = 1.0 / (tokens * devices * TOP / EXPERTS)
    spec = whole()
    params = pltpu.CompilerParams(vmem_limit_bytes=VMEM_GRANT)
    package = pltpu.VMEM((tokens + META, WIDTH), jnp.bfloat16)
    own, sent = pl.pallas_call(
        collect_kernel,
        out_shape=(package, package),
        in_specs=[pl.BlockSpec(memory_space=pltpu.HBM)] * 5,
        out_specs=(spec, spec),
        scratch_shapes=[
            pltpu.VMEM((TOP, tokens), jnp.int32),
            pltpu.VMEM((1, tokens), jnp.float32),
            pltpu.VMEM((1, tokens), jnp.int32),
            pltpu.SemaphoreType.DMA((5,)),
        ],
        compiler_params=pltpu.CompilerParams(vmem_limit_bytes=COLLECT_GRANT),
        name="collect",
    )(
        features,
        gradients,
        route_ids.T,
        gate_share.reshape(1, tokens),
        token_mask.reshape(1, tokens),
    )
    far = shards // FACTORS
    got = lax.ppermute(sent, "dp", [(i, (i + far) % shards) for i in range(shards)])
    chips = far // owners

    def pack(*packages):
        block = pltpu.VMEM((len(packages) * CAP, WIDTH), jnp.bfloat16)
        return pl.pallas_call(
            functools.partial(pack_kernel, len(packages)),
            out_shape=(block,) * EXPERTS,
            in_specs=[spec] * len(packages),
            out_specs=(spec,) * EXPERTS,
            compiler_params=params,
            name="pack",
        )(*packages)

    def deliver(blocks):
        arrived = [blocks[0]]
        for step in range(1, EXPERTS):
            apart = step // chips * shards + step % chips * owners
            arrived.append(lax.ppermute(blocks[step], AXES, [(i, i ^ apart) for i in range(devices)]))
        return arrived

    received = deliver(pack(own)) + deliver(pack(got))
    mine = pl.pallas_call(
        gram_kernel,
        out_shape=pltpu.VMEM((BLOCK, BLOCK), jnp.float32),
        in_specs=[spec] * len(received),
        out_specs=spec,
        compiler_params=params,
        name="gram",
    )(*received)
    other = lax.ppermute(mine, "dp", [(i, i ^ 1) for i in range(shards)])
    rows = pl.pallas_call(
        functools.partial(newton_kernel, load_inverse, owners, shards),
        out_shape=pltpu.VMEM((BLOCK // owners, BLOCK), jnp.float32),
        in_specs=[pl.BlockSpec(memory_space=pltpu.SMEM), spec, spec],
        out_specs=spec,
        compiler_params=params,
        name="newton",
    )(damping.reshape(-1, FACTORS).T, mine, other)
    sent = jnp.concatenate([rows.astype(jnp.float16)] * experts_axis, axis=0)
    lanes = range(owners)
    same_core = [
        [e * shards + i + c for e in range(experts_axis) for i in range(0, shards, owners)]
        for c in lanes
    ]
    gathered = lax.all_to_all(
        sent, AXES, split_axis=0, concat_axis=0, tiled=True, axis_index_groups=same_core
    )
    result = jax.ShapeDtypeStruct((EXPERTS, NBLK, BLOCK // shards, BLOCK), jnp.float32)
    return pl.pallas_call(
        decode_kernel,
        out_shape=(result, result),
        in_specs=[spec],
        out_specs=(spec, spec),
        compiler_params=params,
        name="decode",
    )(gathered.astype(jnp.float32))


def slot_table(route_ids, capacity):
    pair_experts = route_ids.reshape(-1)
    onehot = (pair_experts[:, None] == jnp.arange(EXPERTS, dtype=jnp.int32)[None, :]).astype(
        jnp.int32
    )
    running = jnp.cumsum(onehot, axis=0)
    position = jnp.sum(onehot * running, axis=1) - 1
    target = pair_experts * capacity + position
    sources = jnp.arange(1, pair_experts.shape[0] + 1, dtype=jnp.int32)
    return jnp.zeros((EXPERTS * capacity,), jnp.int32).at[target].set(sources)


def newton_rows(rows_now, matrix, whole_now):
    left_product = jnp.einsum("eirk,eikc->eirc", rows_now, matrix, precision=lax.Precision.HIGHEST)
    return 2.0 * rows_now - jnp.einsum(
        "eirk,eikc->eirc", left_product, whole_now, precision=lax.Precision.HIGHEST
    )


def first_iterate(matrix, identity, inverse_bound):
    bound_scale = inverse_bound[:, :, None, None]
    return 2.0 * bound_scale * identity - bound_scale * bound_scale * matrix


def shared(features, gradients, route_ids, gate_share, token_mask, damping):
    tokens_here = features.shape[0]
    capacity = CAP
    blocks = 2 * NBLK
    kept_mask = token_mask.astype(jnp.float32)
    weight_pair = jnp.stack([gate_share, 1.0 - gate_share], axis=1) * kept_mask[:, None]
    kept_rows = features * token_mask.astype(jnp.bfloat16)[:, None]
    pair_grads = (gradients[:, None, :].astype(jnp.float32) * weight_pair[:, :, None]).astype(
        jnp.bfloat16
    )
    repeated = jnp.broadcast_to(kept_rows[:, None, :], pair_grads.shape)
    pair_rows = jnp.concatenate([repeated, pair_grads], axis=2).reshape(
        tokens_here * TOP, 2 * WIDTH
    )
    padded = jnp.concatenate([jnp.zeros((1, 2 * WIDTH), jnp.bfloat16), pair_rows], axis=0)
    buffer = jnp.take(padded, slot_table(route_ids, capacity), axis=0).reshape(
        EXPERTS, capacity, blocks, BLOCK
    )
    load_inverse = 1.0 / (
        tokens_here * lax.axis_size("expert") * lax.axis_size("dp") * TOP / EXPERTS
    )
    received = lax.all_to_all(buffer, "expert", split_axis=0, concat_axis=1, tiled=True)
    gram_blocks = (
        jnp.einsum("erib,eric->eibc", received, received, preferred_element_type=jnp.float32)
        * load_inverse
    )
    damping_flat = damping.reshape(damping.shape[0], blocks)[:, :, None, None]
    rows_share = BLOCK // lax.axis_size("dp")
    row_start = lax.axis_index("dp") * rows_share
    identity = jnp.eye(BLOCK, dtype=jnp.float32)
    summed = lax.psum(gram_blocks, "dp")
    matrix = summed + damping_flat * identity
    largest_sum = jnp.max(jnp.sum(jnp.abs(matrix), axis=3), axis=2)
    inverse_bound = 1.0 / largest_sum
    iterate_one = first_iterate(matrix, identity, inverse_bound)
    iterate_two = newton_rows(iterate_one, matrix, iterate_one)
    second_rows = lax.dynamic_slice_in_dim(iterate_two, row_start, rows_share, 2)
    third_rows = newton_rows(second_rows, matrix, iterate_two)
    act_rows = third_rows[:, :NBLK]
    grad_rows = third_rows[:, NBLK:]
    return (
        lax.all_gather(act_rows, "expert", axis=0, tiled=True),
        lax.all_gather(grad_rows, "expert", axis=0, tiled=True),
    )


def solution(mesh):
    placed = (
        P(("expert", "dp"), None),
        P(("expert", "dp"), None),
        P(("expert", "dp"), None),
        P(("expert", "dp")),
        P(("expert", "dp")),
        P("expert", None, None),
    )
    paired = mesh.shape["expert"] * mesh.shape["dp"] == 2 * MATRICES
    return jax.shard_map(
        owned if paired else shared,
        mesh=mesh,
        in_specs=placed,
        out_specs=(P(None, None, "dp", None), P(None, None, "dp", None)),
        check_vma=False,
    )
```

```python
import functools

import jax
import jax.numpy as jnp
from jax import lax
from jax.experimental import pallas as pl
from jax.experimental.pallas import tpu as pltpu
from jax.sharding import PartitionSpec as P


EXPERTS = 8
TOP = 2
BLOCK = 512
NBLK = 1
CAP = 64
WIDTH = 512
FACTORS = 2 * NBLK
MATRICES = EXPERTS * FACTORS
OWNERS = 2
LANES = 128
TILES = BLOCK // LANES
UPPER = [(top, left) for top in range(TILES) for left in range(top, TILES)]
VMEM_GRANT = 16 * 2**20
COLLECT_GRANT = 60 * 2**20
SENT_SCALE = 2.0**14
AXES = ("expert", "dp")


def whole(*shape):
    return pl.BlockSpec(memory_space=pltpu.VMEM)


META = 8
EARLY = (0, 7,3,6,5)
LATE = (0, 1,2,4,7,3,6,5)


def chip_of(expert_shard, shard, shards):
    chips = shards // FACTORS // OWNERS
    return expert_shard * chips + lax.rem(shard, chips * OWNERS) // OWNERS


def collect_kernel(features, gradients, routes, share, mask, own, sent, ids, weight, kept, sems):
    tokens = features.shape[0]
    lower = lax.axis_index("dp") < lax.axis_size("dp") // FACTORS
    small = [
        pltpu.make_async_copy(routes, ids, sems.at[2]),
        pltpu.make_async_copy(share, weight, sems.at[3]),
        pltpu.make_async_copy(mask, kept, sems.at[4]),
    ]
    for copy in small:
        copy.start()

    def tokens_in(source, target, sem):
        return pltpu.make_async_copy(source, target.at[0:tokens], sems.at[sem])

    @pl.when(lower)
    def _():
        tokens_in(gradients, sent, 0).start()
        tokens_in(features, own, 1).start()

    @pl.when(jnp.logical_not(lower))
    def _():
        tokens_in(features, sent, 0).start()
        tokens_in(gradients, own, 1).start()

    for copy in small:
        copy.wait()
    high = weight[...].astype(jnp.bfloat16).astype(jnp.float32)
    rest = weight[...] - high
    middle = rest.astype(jnp.bfloat16).astype(jnp.float32)
    low = rest - middle
    first = jnp.concatenate(
        [
            ids[0:1, :].astype(jnp.float32),
            ids[1:2, :].astype(jnp.float32),
            kept[...].astype(jnp.float32),
            high,
        ],
        axis=1,
    )
    second = jnp.concatenate([middle, low, jnp.zeros_like(low), jnp.zeros_like(low)], axis=1)
    row = lax.broadcasted_iota(jnp.int32, (META, WIDTH), 0)
    meta = jnp.where(row == 0, first, jnp.where(row == 1, second, 0.0)).astype(jnp.bfloat16)
    own[tokens : tokens + META, :] = meta
    sent[tokens : tokens + META, :] = meta
    tokens_in(features, sent, 0).wait()
    tokens_in(features, own, 1).wait()


def pack_kernel(plan, *refs):
    inputs, outputs = refs[: len(plan)], refs[len(plan) :]
    tokens = inputs[0].shape[0] - META
    shard, shards = lax.axis_index("dp"), lax.axis_size("dp")
    lower = shard < shards // FACTORS
    chip = chip_of(lax.axis_index("expert"), shard, shards)
    expert = lax.broadcasted_iota(jnp.int32, (EXPERTS, tokens), 0)
    earlier = lax.broadcasted_iota(jnp.int32, (tokens, tokens), 0) < lax.broadcasted_iota(
        jnp.int32, (tokens, tokens), 1
    )
    earlier = jnp.where(earlier, 1.0, 0.0).astype(jnp.bfloat16)
    for package, places in zip(inputs, plan):
        slot = lax.broadcasted_iota(jnp.int32, (len(places) * CAP, tokens), 0)
        meta = package[tokens : tokens + META, :].astype(jnp.float32)

        def part(row, index):
            return meta[row : row + 1, index * tokens : (index + 1) * tokens]

        first = part(0, 0).astype(jnp.int32) ^ chip
        second = part(0, 1).astype(jnp.int32) ^ chip
        kept = part(0, 2)
        share = (part(0, 3) + part(1, 0)) + part(1, 1)
        is_first, is_second = expert == first, expert == second
        member = jnp.where(is_first | is_second, 1.0, 0.0).astype(jnp.bfloat16)
        position = jnp.dot(member, earlier, preferred_element_type=jnp.float32)
        wide = package[0:tokens, :].astype(jnp.float32)

        def picked(chosen, named):
            spot = jnp.sum(jnp.where(chosen, position, 0.0), axis=0, keepdims=True)
            base = jnp.full_like(named, -len(places) * CAP - CAP)
            for rank, (apart, _, _) in enumerate(places):
                base = jnp.where(named == apart, rank * CAP, base)
            hit = slot == base + spot.astype(jnp.int32)
            return jnp.where(hit, 1.0, 0.0).astype(jnp.bfloat16)

        def weighted(weight):
            weight = jnp.where(lower, kept, weight * kept)
            column = jnp.transpose(jnp.broadcast_to(weight, (tokens, tokens)))
            column = jnp.concatenate([column] * (WIDTH // tokens), axis=1)
            return (wide * column).astype(jnp.bfloat16)

        picks = jnp.concatenate([picked(is_first, first), picked(is_second, second)], axis=1)
        pairs = jnp.concatenate([weighted(share), weighted(1.0 - share)], axis=0)
        rows = jnp.dot(picks, pairs, preferred_element_type=jnp.float32).astype(jnp.bfloat16)
        for rank, (_, index, row) in enumerate(places):
            outputs[index][row : row + CAP, :] = rows[rank * CAP : (rank + 1) * CAP]


def gram_kernel(*refs):
    rows = jnp.concatenate([ref[...] for ref in refs[:-1]], axis=0)
    gram = lax.dot_general(
        rows, rows, (((0,), (0,)), ((), ())), preferred_element_type=jnp.float32
    )
    for index, (top, left) in enumerate(UPPER):
        refs[-1][index] = gram[
            top * LANES : (top + 1) * LANES, left * LANES : (left + 1) * LANES
        ]


def split(value):
    high = value.astype(jnp.bfloat16)
    return high, (value - high.astype(jnp.float32)).astype(jnp.bfloat16)


def product(left, right):
    (left_high, left_low), (right_high, right_low) = left, right

    def dot(a, b):
        return jnp.dot(a, b, preferred_element_type=jnp.float32)

    return dot(left_high, right_high) + (dot(left_high, right_low) + dot(left_low, right_high))


def newton_kernel(load_inverse, owners, shards, damping, mine, other, out):
    shard = lax.axis_index("dp")
    core = lax.rem(shard, owners)
    factor = shard // (shards // FACTORS)
    expert = lax.rem(shard, shards // FACTORS) // owners
    place = lax.broadcasted_iota(jnp.int32, (BLOCK, BLOCK), 0)
    identity = jnp.where(place == lax.broadcasted_iota(jnp.int32, (BLOCK, BLOCK), 1), 1.0, 0.0)
    tiles = {}
    for index, (top, left) in enumerate(UPPER):
        tiles[top, left] = mine[index] + other[index]
        if top != left:
            tiles[left, top] = jnp.transpose(tiles[top, left])
    gram = jnp.concatenate(
        [
            jnp.concatenate([tiles[top, left] for left in range(TILES)], axis=1)
            for top in range(TILES)
        ],
        axis=0,
    )
    matrix = gram * load_inverse + damping[factor, expert] * identity
    bound = jnp.max(jnp.sum(jnp.abs(matrix), axis=0, keepdims=True), axis=1, keepdims=True)
    scale = 1.0 / bound
    error = identity - scale * matrix
    parts = split(error)
    square = split(product(parts, parts))
    start = (identity + error).reshape(shards // owners, owners, BLOCK // shards, BLOCK)
    rows = start[:, 0]
    for turn in range(1, owners):
        rows = jnp.where(core == turn, start[:, turn], rows)
    rows = rows.reshape(BLOCK // owners, BLOCK)
    rows = rows + product(split(rows), square)
    last = rows + product(split(product(split(rows), square)), square)
    last = (scale * SENT_SCALE) * last
    encode(core, shards, owners, last, out)


def encode(core, shards, owners, rows, out):
    share = BLOCK // shards
    out[...] = rows
    turns = shards // owners
    starts = [turn * owners * share // LANES * LANES for turn in range(turns)]
    tile = jnp.concatenate(
        [
            rows[turn * share : (turn + 1) * share, start : start + LANES]
            for turn, start in enumerate(starts)
        ],
        axis=0,
    )
    place = lax.broadcasted_iota(jnp.int32, tile.shape, 0)
    row = lax.rem(place, share)
    first = lax.rem(place // share * (owners * share), LANES) + core * share
    column = lax.broadcasted_iota(jnp.int32, tile.shape, 1) - first
    high = tile.astype(jnp.bfloat16).astype(jnp.float32)
    low = tile - high
    beside = pltpu.roll(low, LANES - 1, 1)
    tile = jnp.where(column == row, high, tile)
    tile = jnp.where((column == row - 1) & (row > 0), beside, tile)
    tile = jnp.where((column == 0) & (row == 2), pltpu.roll(low, 2, 0), tile)
    for turn, start in enumerate(starts):
        part = slice(turn * share, (turn + 1) * share)
        out[part, start : start + LANES] = tile[part]


def decode_kernel(rows, act, grad):
    groups, share = lax.axis_size("expert"), act.shape[2]
    first = lax.axis_index("dp") * share
    start = pl.multiple_of(first // LANES * LANES, LANES)

    def by_factor(value):
        value = value.reshape(groups, FACTORS, EXPERTS // groups, share, value.shape[-1])
        return (
            (out, value[:, factor].reshape(EXPERTS, share, value.shape[-1]))
            for out, factor in ((act, 0), (grad, 1))
        )

    for out, value in by_factor(rows[...] * (1.0 / SENT_SCALE)):
        out[:, 0] = value
    total = rows.shape[0]
    tile = rows[:, pl.ds(start, LANES)] * (1.0 / SENT_SCALE)
    row = lax.rem(lax.broadcasted_iota(jnp.int32, (total, LANES), 0), share)
    column = lax.broadcasted_iota(jnp.int32, (total, LANES), 1) - (first - start)

    def moved(down, right):
        value = tile
        if down:
            value = pltpu.roll(value, down % total, 0)
        if right:
            value = pltpu.roll(value, right % LANES, 1)
        return value

    fixed = jnp.where(column == row, tile + jnp.where(row > 0, moved(0, 1), moved(-2, 0)), tile)
    fixed = jnp.where((column == row - 1) & (row > 0), moved(1, -1), fixed)
    fixed = jnp.where((column == 0) & (row == 2), moved(2, -2), fixed)
    for out, value in by_factor(fixed):
        out[:, 0, :, pl.ds(start, LANES)] = value


def owned(features, gradients, route_ids, gate_share, token_mask, damping):
    tokens = features.shape[0]
    experts_axis, shards = lax.axis_size("expert"), lax.axis_size("dp")
    devices = experts_axis * shards
    owners = devices // MATRICES
    load_inverse = 1.0 / (tokens * devices * TOP / EXPERTS)
    spec = whole()
    params = pltpu.CompilerParams(vmem_limit_bytes=VMEM_GRANT)
    package = pltpu.VMEM((tokens + META, WIDTH), jnp.bfloat16)
    own, sent = pl.pallas_call(
        collect_kernel,
        out_shape=(package, package),
        in_specs=[pl.BlockSpec(memory_space=pltpu.HBM)] * 5,
        out_specs=(spec, spec),
        scratch_shapes=[
            pltpu.VMEM((TOP, tokens), jnp.int32),
            pltpu.VMEM((1, tokens), jnp.float32),
            pltpu.VMEM((1, tokens), jnp.int32),
            pltpu.SemaphoreType.DMA((5,)),
        ],
        compiler_params=pltpu.CompilerParams(vmem_limit_bytes=COLLECT_GRANT),
        name="collect",
    )(
        features,
        gradients,
        route_ids.T,
        gate_share.reshape(1, tokens),
        token_mask.reshape(1, tokens),
    )
    far = shards // FACTORS
    chips = far // owners

    def pack(packages, wanted):
        plan, sizes = [[] for _ in packages], []
        for index, (apart, sources) in enumerate(wanted):
            for order, source in enumerate(sources):
                plan[source].append((apart, index, order * CAP))
            sizes.append(len(sources) * CAP)
        return pl.pallas_call(
            functools.partial(pack_kernel, plan),
            out_shape=[pltpu.VMEM((size, WIDTH), jnp.bfloat16) for size in sizes],
            in_specs=[spec] * len(packages),
            out_specs=[spec] * len(sizes),
            compiler_params=params,
            name="pack",
        )(*packages)

    def deliver(block, step):
        if step == 0:
            return block
        apart = step // chips * shards + step % chips * owners
        return lax.ppermute(block, AXES, [(i, i ^ apart) for i in range(devices)])

    early = [(step, (0,)) for step in EARLY]
    late = [(step, (1,) if step in EARLY else (0, 1)) for step in LATE]
    got = lax.ppermute(sent, "dp", [(i, (i + far) % shards) for i in range(shards)])
    blocks = pack([own], early)
    received = []
    for block, (step, _) in zip(blocks, early):
        received.append(deliver(block, step))
    blocks = pack([own, got], late)
    for block, (step, _) in zip(blocks, late):
        received.append(deliver(block, step))
    mine = pl.pallas_call(
        gram_kernel,
        out_shape=pltpu.VMEM((len(UPPER), LANES, LANES), jnp.float32),
        in_specs=[spec] * len(received),
        out_specs=spec,
        compiler_params=params,
        name="gram",
    )(*received)
    other = lax.ppermute(mine, "dp", [(i, i ^ 1) for i in range(shards)])
    rows = pl.pallas_call(
        functools.partial(newton_kernel, load_inverse, owners, shards),
        out_shape=pltpu.VMEM((BLOCK // owners, BLOCK), jnp.float32),
        in_specs=[pl.BlockSpec(memory_space=pltpu.SMEM), spec, spec],
        out_specs=spec,
        compiler_params=params,
        name="newton",
    )(damping.reshape(-1, FACTORS).T, mine, other)
    sent = jnp.concatenate([rows.astype(jnp.float16)] * experts_axis, axis=0)
    lanes = range(owners)
    same_core = [
        [e * shards + i + c for e in range(experts_axis) for i in range(0, shards, owners)]
        for c in lanes
    ]
    gathered = lax.all_to_all(
        sent, AXES, split_axis=0, concat_axis=0, tiled=True, axis_index_groups=same_core
    )
    result = jax.ShapeDtypeStruct((EXPERTS, NBLK, BLOCK // shards, BLOCK), jnp.float32)
    return pl.pallas_call(
        decode_kernel,
        out_shape=(result, result),
        in_specs=[spec],
        out_specs=(spec, spec),
        compiler_params=params,
        name="decode",
    )(gathered.astype(jnp.float32))


def slot_table(route_ids, capacity):
    pair_experts = route_ids.reshape(-1)
    onehot = (pair_experts[:, None] == jnp.arange(EXPERTS, dtype=jnp.int32)[None, :]).astype(
        jnp.int32
    )
    running = jnp.cumsum(onehot, axis=0)
    position = jnp.sum(onehot * running, axis=1) - 1
    target = pair_experts * capacity + position
    sources = jnp.arange(1, pair_experts.shape[0] + 1, dtype=jnp.int32)
    return jnp.zeros((EXPERTS * capacity,), jnp.int32).at[target].set(sources)


def newton_rows(rows_now, matrix, whole_now):
    left_product = jnp.einsum("eirk,eikc->eirc", rows_now, matrix, precision=lax.Precision.HIGHEST)
    return 2.0 * rows_now - jnp.einsum(
        "eirk,eikc->eirc", left_product, whole_now, precision=lax.Precision.HIGHEST
    )


def first_iterate(matrix, identity, inverse_bound):
    bound_scale = inverse_bound[:, :, None, None]
    return 2.0 * bound_scale * identity - bound_scale * bound_scale * matrix


def shared(features, gradients, route_ids, gate_share, token_mask, damping):
    tokens_here = features.shape[0]
    capacity = CAP
    blocks = 2 * NBLK
    kept_mask = token_mask.astype(jnp.float32)
    weight_pair = jnp.stack([gate_share, 1.0 - gate_share], axis=1) * kept_mask[:, None]
    kept_rows = features * token_mask.astype(jnp.bfloat16)[:, None]
    pair_grads = (gradients[:, None, :].astype(jnp.float32) * weight_pair[:, :, None]).astype(
        jnp.bfloat16
    )
    repeated = jnp.broadcast_to(kept_rows[:, None, :], pair_grads.shape)
    pair_rows = jnp.concatenate([repeated, pair_grads], axis=2).reshape(
        tokens_here * TOP, 2 * WIDTH
    )
    padded = jnp.concatenate([jnp.zeros((1, 2 * WIDTH), jnp.bfloat16), pair_rows], axis=0)
    buffer = jnp.take(padded, slot_table(route_ids, capacity), axis=0).reshape(
        EXPERTS, capacity, blocks, BLOCK
    )
    load_inverse = 1.0 / (
        tokens_here * lax.axis_size("expert") * lax.axis_size("dp") * TOP / EXPERTS
    )
    received = lax.all_to_all(buffer, "expert", split_axis=0, concat_axis=1, tiled=True)
    gram_blocks = (
        jnp.einsum("erib,eric->eibc", received, received, preferred_element_type=jnp.float32)
        * load_inverse
    )
    damping_flat = damping.reshape(damping.shape[0], blocks)[:, :, None, None]
    rows_share = BLOCK // lax.axis_size("dp")
    row_start = lax.axis_index("dp") * rows_share
    identity = jnp.eye(BLOCK, dtype=jnp.float32)
    summed = lax.psum(gram_blocks, "dp")
    matrix = summed + damping_flat * identity
    largest_sum = jnp.max(jnp.sum(jnp.abs(matrix), axis=3), axis=2)
    inverse_bound = 1.0 / largest_sum
    iterate_one = first_iterate(matrix, identity, inverse_bound)
    iterate_two = newton_rows(iterate_one, matrix, iterate_one)
    second_rows = lax.dynamic_slice_in_dim(iterate_two, row_start, rows_share, 2)
    third_rows = newton_rows(second_rows, matrix, iterate_two)
    act_rows = third_rows[:, :NBLK]
    grad_rows = third_rows[:, NBLK:]
    return (
        lax.all_gather(act_rows, "expert", axis=0, tiled=True),
        lax.all_gather(grad_rows, "expert", axis=0, tiled=True),
    )


def solution(mesh):
    placed = (
        P(("expert", "dp"), None),
        P(("expert", "dp"), None),
        P(("expert", "dp"), None),
        P(("expert", "dp")),
        P(("expert", "dp")),
        P("expert", None, None),
    )
    paired = mesh.shape["expert"] * mesh.shape["dp"] == 2 * MATRICES
    return jax.shard_map(
        owned if paired else shared,
        mesh=mesh,
        in_specs=placed,
        out_specs=(P(None, None, "dp", None), P(None, None, "dp", None)),
        check_vma=False,
    )
```

```python
import functools

import jax
import jax.numpy as jnp
from jax import lax
from jax.experimental import pallas as pl
from jax.experimental.pallas import tpu as pltpu
from jax.sharding import PartitionSpec as P


EXPERTS = 8
TOP = 2
BLOCK = 512
NBLK = 1
CAP = 64
WIDTH = 512
FACTORS = 2 * NBLK
MATRICES = EXPERTS * FACTORS
OWNERS = 2
LANES = 128
TILES = BLOCK // LANES
UPPER = [(top, left) for top in range(TILES) for left in range(top, TILES)]
VMEM_GRANT = 16 * 2**20
COLLECT_GRANT = 60 * 2**20
SENT_SCALE = 2.0**14
AXES = ("expert", "dp")


def whole(*shape):
    return pl.BlockSpec(memory_space=pltpu.VMEM)


META = 8
EARLY = (0, 7, 3, 6, 5)
LATE = (0, 1, 2, 4, 7, 3, 6, 5)


def chip_of(expert_shard, shard, shards):
    chips = shards // FACTORS // OWNERS
    return expert_shard * chips + lax.rem(shard, chips * OWNERS) // OWNERS


def collect_kernel(features, gradients, routes, share, mask, own, sent, ids, weight, kept, sems):
    tokens = features.shape[0]
    lower = lax.axis_index("dp") < lax.axis_size("dp") // FACTORS
    small = [
        pltpu.make_async_copy(routes, ids, sems.at[2]),
        pltpu.make_async_copy(share, weight, sems.at[3]),
        pltpu.make_async_copy(mask, kept, sems.at[4]),
    ]
    for copy in small:
        copy.start()

    def tokens_in(source, target, sem):
        return pltpu.make_async_copy(source, target.at[0:tokens], sems.at[sem])

    @pl.when(lower)
    def _():
        tokens_in(gradients, sent, 0).start()
        tokens_in(features, own, 1).start()

    @pl.when(jnp.logical_not(lower))
    def _():
        tokens_in(features, sent, 0).start()
        tokens_in(gradients, own, 1).start()

    for copy in small:
        copy.wait()
    high = weight[...].astype(jnp.bfloat16).astype(jnp.float32)
    rest = weight[...] - high
    middle = rest.astype(jnp.bfloat16).astype(jnp.float32)
    low = rest - middle
    first = jnp.concatenate(
        [
            ids[0:1, :].astype(jnp.float32),
            ids[1:2, :].astype(jnp.float32),
            kept[...].astype(jnp.float32),
            high,
        ],
        axis=1,
    )
    second = jnp.concatenate([middle, low, jnp.zeros_like(low), jnp.zeros_like(low)], axis=1)
    row = lax.broadcasted_iota(jnp.int32, (META, WIDTH), 0)
    meta = jnp.where(row == 0, first, jnp.where(row == 1, second, 0.0)).astype(jnp.bfloat16)
    own[tokens : tokens + META, :] = meta
    sent[tokens : tokens + META, :] = meta
    tokens_in(features, sent, 0).wait()
    tokens_in(features, own, 1).wait()


def pack_kernel(plan, *refs):
    inputs, outputs = refs[: len(plan)], refs[len(plan) :]
    tokens = inputs[0].shape[0] - META
    shard, shards = lax.axis_index("dp"), lax.axis_size("dp")
    lower = shard < shards // FACTORS
    chip = chip_of(lax.axis_index("expert"), shard, shards)
    expert = lax.broadcasted_iota(jnp.int32, (EXPERTS, tokens), 0)
    earlier = lax.broadcasted_iota(jnp.int32, (tokens, tokens), 0) < lax.broadcasted_iota(
        jnp.int32, (tokens, tokens), 1
    )
    earlier = jnp.where(earlier, 1.0, 0.0).astype(jnp.bfloat16)
    for package, places in zip(inputs, plan):
        slot = lax.broadcasted_iota(jnp.int32, (len(places) * CAP, tokens), 0)
        meta = package[tokens : tokens + META, :].astype(jnp.float32)

        def part(row, index):
            return meta[row : row + 1, index * tokens : (index + 1) * tokens]

        first = part(0, 0).astype(jnp.int32) ^ chip
        second = part(0, 1).astype(jnp.int32) ^ chip
        kept = part(0, 2)
        share = (part(0, 3) + part(1, 0)) + part(1, 1)
        is_first, is_second = expert == first, expert == second
        member = jnp.where(is_first | is_second, 1.0, 0.0).astype(jnp.bfloat16)
        position = jnp.dot(member, earlier, preferred_element_type=jnp.float32)
        wide = package[0:tokens, :].astype(jnp.float32)

        def picked(chosen, named):
            spot = jnp.sum(jnp.where(chosen, position, 0.0), axis=0, keepdims=True)
            base = jnp.full_like(named, -len(places) * CAP - CAP)
            for rank, (apart, _, _) in enumerate(places):
                base = jnp.where(named == apart, rank * CAP, base)
            hit = slot == base + spot.astype(jnp.int32)
            return jnp.where(hit, 1.0, 0.0).astype(jnp.bfloat16)

        def weighted(weight):
            weight = jnp.where(lower, kept, weight * kept)
            column = jnp.transpose(jnp.broadcast_to(weight, (tokens, tokens)))
            column = jnp.concatenate([column] * (WIDTH // tokens), axis=1)
            return (wide * column).astype(jnp.bfloat16)

        picks = jnp.concatenate([picked(is_first, first), picked(is_second, second)], axis=1)
        pairs = jnp.concatenate([weighted(share), weighted(1.0 - share)], axis=0)
        rows = jnp.dot(picks, pairs, preferred_element_type=jnp.float32).astype(jnp.bfloat16)
        for rank, (_, index, row) in enumerate(places):
            outputs[index][row : row + CAP, :] = rows[rank * CAP : (rank + 1) * CAP]


def gram_kernel(*refs):
    rows = jnp.concatenate([ref[...] for ref in refs[:-1]], axis=0)
    gram = lax.dot_general(
        rows, rows, (((0,), (0,)), ((), ())), preferred_element_type=jnp.float32
    )
    for index, (top, left) in enumerate(UPPER):
        refs[-1][index] = gram[
            top * LANES : (top + 1) * LANES, left * LANES : (left + 1) * LANES
        ]


def split(value):
    high = value.astype(jnp.bfloat16)
    return high, (value - high.astype(jnp.float32)).astype(jnp.bfloat16)


def product(left, right):
    (left_high, left_low), (right_high, right_low) = left, right

    def dot(a, b):
        return jnp.dot(a, b, preferred_element_type=jnp.float32)

    return dot(left_high, right_high) + (dot(left_high, right_low) + dot(left_low, right_high))


def newton_kernel(load_inverse, owners, shards, damping, mine, other, out):
    shard = lax.axis_index("dp")
    core = lax.rem(shard, owners)
    factor = shard // (shards // FACTORS)
    expert = lax.rem(shard, shards // FACTORS) // owners
    place = lax.broadcasted_iota(jnp.int32, (BLOCK, BLOCK), 0)
    identity = jnp.where(place == lax.broadcasted_iota(jnp.int32, (BLOCK, BLOCK), 1), 1.0, 0.0)
    tiles = {}
    for index, (top, left) in enumerate(UPPER):
        tiles[top, left] = mine[index] + other[index]
        if top != left:
            tiles[left, top] = jnp.transpose(tiles[top, left])
    gram = jnp.concatenate(
        [
            jnp.concatenate([tiles[top, left] for left in range(TILES)], axis=1)
            for top in range(TILES)
        ],
        axis=0,
    )
    matrix = gram * load_inverse + damping[factor, expert] * identity
    bound = jnp.max(jnp.sum(jnp.abs(matrix), axis=0, keepdims=True), axis=1, keepdims=True)
    scale = 1.0 / bound
    error = identity - scale * matrix
    parts = split(error)
    cross = jnp.dot(parts[0], parts[1], preferred_element_type=jnp.float32)
    square = jnp.dot(parts[0], parts[0], preferred_element_type=jnp.float32)
    square = split(square + (cross + jnp.transpose(cross)))
    start = (identity + error).reshape(shards // owners, owners, BLOCK // shards, BLOCK)
    rows = start[:, 0]
    for turn in range(1, owners):
        rows = jnp.where(core == turn, start[:, turn], rows)
    rows = rows.reshape(BLOCK // owners, BLOCK)
    rows = rows + product(split(rows), square)
    last = rows + product(split(product(split(rows), square)), square)
    last = (scale * SENT_SCALE) * last
    encode(core, shards, owners, last, out)


def encode(core, shards, owners, rows, out):
    share = BLOCK // shards
    out[...] = rows
    turns = shards // owners
    starts = [turn * owners * share // LANES * LANES for turn in range(turns)]
    tile = jnp.concatenate(
        [
            rows[turn * share : (turn + 1) * share, start : start + LANES]
            for turn, start in enumerate(starts)
        ],
        axis=0,
    )
    place = lax.broadcasted_iota(jnp.int32, tile.shape, 0)
    row = lax.rem(place, share)
    first = lax.rem(place // share * (owners * share), LANES) + core * share
    column = lax.broadcasted_iota(jnp.int32, tile.shape, 1) - first
    high = tile.astype(jnp.bfloat16).astype(jnp.float32)
    low = tile - high
    beside = pltpu.roll(low, LANES - 1, 1)
    tile = jnp.where(column == row, high, tile)
    tile = jnp.where((column == row - 1) & (row > 0), beside, tile)
    tile = jnp.where((column == 0) & (row == 2), pltpu.roll(low, 2, 0), tile)
    for turn, start in enumerate(starts):
        part = slice(turn * share, (turn + 1) * share)
        out[part, start : start + LANES] = tile[part]


def decode_kernel(rows, act, grad, results, sems):
    groups, share = lax.axis_size("expert"), act.shape[2]
    first = lax.axis_index("dp") * share
    start = pl.multiple_of(first // LANES * LANES, LANES)
    total = rows.shape[0]
    tile = rows[:, pl.ds(start, LANES)]
    row = lax.rem(lax.broadcasted_iota(jnp.int32, (total, LANES), 0), share)
    column = lax.broadcasted_iota(jnp.int32, (total, LANES), 1) - (first - start)

    def moved(down, right):
        value = tile
        if down:
            value = pltpu.roll(value, down % total, 0)
        if right:
            value = pltpu.roll(value, right % LANES, 1)
        return value

    fixed = jnp.where(column == row, tile + jnp.where(row > 0, moved(0, 1), moved(-2, 0)), tile)
    fixed = jnp.where((column == row - 1) & (row > 0), moved(1, -1), fixed)
    fixed = jnp.where((column == 0) & (row == 2), moved(2, -2), fixed)

    def of_factor(value, factor):
        value = value.reshape(groups, FACTORS, EXPERTS // groups, share, value.shape[-1])
        return value[:, factor].reshape(EXPERTS, share, value.shape[-1])

    copies = []
    for factor, out in ((0, act), (1, grad)):
        results[factor] = of_factor(rows[...], factor)
        results[factor, :, :, pl.ds(start, LANES)] = of_factor(fixed, factor)
        copies.append(pltpu.make_async_copy(results.at[factor], out.at[:, 0], sems.at[factor]))
        copies[-1].start()
    for copy in copies:
        copy.wait()


def owned(features, gradients, route_ids, gate_share, token_mask, damping):
    tokens = features.shape[0]
    experts_axis, shards = lax.axis_size("expert"), lax.axis_size("dp")
    devices = experts_axis * shards
    owners = devices // MATRICES
    load_inverse = 1.0 / (tokens * devices * TOP / EXPERTS)
    spec = whole()
    params = pltpu.CompilerParams(vmem_limit_bytes=VMEM_GRANT)
    package = pltpu.VMEM((tokens + META, WIDTH), jnp.bfloat16)
    own, sent = pl.pallas_call(
        collect_kernel,
        out_shape=(package, package),
        in_specs=[pl.BlockSpec(memory_space=pltpu.HBM)] * 5,
        out_specs=(spec, spec),
        scratch_shapes=[
            pltpu.VMEM((TOP, tokens), jnp.int32),
            pltpu.VMEM((1, tokens), jnp.float32),
            pltpu.VMEM((1, tokens), jnp.int32),
            pltpu.SemaphoreType.DMA((5,)),
        ],
        compiler_params=pltpu.CompilerParams(vmem_limit_bytes=COLLECT_GRANT),
        name="collect",
    )(
        features,
        gradients,
        route_ids.T,
        gate_share.reshape(1, tokens),
        token_mask.reshape(1, tokens),
    )
    far = shards // FACTORS
    chips = far // owners

    def pack(packages, wanted):
        plan, sizes = [[] for _ in packages], []
        for index, (apart, sources) in enumerate(wanted):
            for order, source in enumerate(sources):
                plan[source].append((apart, index, order * CAP))
            sizes.append(len(sources) * CAP)
        return pl.pallas_call(
            functools.partial(pack_kernel, plan),
            out_shape=[pltpu.VMEM((size, WIDTH), jnp.bfloat16) for size in sizes],
            in_specs=[spec] * len(packages),
            out_specs=[spec] * len(sizes),
            compiler_params=params,
            name="pack",
        )(*packages)

    def deliver(block, step):
        if step == 0:
            return block
        apart = step // chips * shards + step % chips * owners
        return lax.ppermute(block, AXES, [(i, i ^ apart) for i in range(devices)])

    early = [(step, (0,)) for step in EARLY]
    late = [(step, (1,) if step in EARLY else (0, 1)) for step in LATE]
    got = lax.ppermute(sent, "dp", [(i, (i + far) % shards) for i in range(shards)])
    blocks = pack([own], early)
    received = []
    for block, (step, _) in zip(blocks, early):
        received.append(deliver(block, step))
    blocks = pack([own, got], late)
    for block, (step, _) in zip(blocks, late):
        received.append(deliver(block, step))
    mine = pl.pallas_call(
        gram_kernel,
        out_shape=pltpu.VMEM((len(UPPER), LANES, LANES), jnp.float32),
        in_specs=[spec] * len(received),
        out_specs=spec,
        compiler_params=params,
        name="gram",
    )(*received)
    other = lax.ppermute(mine, "dp", [(i, i ^ 1) for i in range(shards)])
    rows = pl.pallas_call(
        functools.partial(newton_kernel, load_inverse, owners, shards),
        out_shape=pltpu.VMEM((BLOCK // owners, BLOCK), jnp.float32),
        in_specs=[pl.BlockSpec(memory_space=pltpu.SMEM), spec, spec],
        out_specs=spec,
        compiler_params=params,
        name="newton",
    )(damping.reshape(-1, FACTORS).T, mine, other)
    sent = jnp.concatenate([rows.astype(jnp.float16)] * experts_axis, axis=0)
    lanes = range(owners)
    same_core = [
        [e * shards + i + c for e in range(experts_axis) for i in range(0, shards, owners)]
        for c in lanes
    ]
    gathered = lax.all_to_all(
        sent, AXES, split_axis=0, concat_axis=0, tiled=True, axis_index_groups=same_core
    )
    result = jax.ShapeDtypeStruct((EXPERTS, NBLK, BLOCK // shards, BLOCK), jnp.float32)
    return pl.pallas_call(
        decode_kernel,
        out_shape=(result, result),
        in_specs=[spec],
        out_specs=(pl.BlockSpec(memory_space=pltpu.HBM),) * FACTORS,
        scratch_shapes=[
            pltpu.VMEM((FACTORS, EXPERTS, BLOCK // shards, BLOCK), jnp.float32),
            pltpu.SemaphoreType.DMA((FACTORS,)),
        ],
        compiler_params=params,
        name="decode",
    )(gathered.astype(jnp.float32) * (1.0 / SENT_SCALE))


def slot_table(route_ids, capacity):
    pair_experts = route_ids.reshape(-1)
    onehot = (pair_experts[:, None] == jnp.arange(EXPERTS, dtype=jnp.int32)[None, :]).astype(
        jnp.int32
    )
    running = jnp.cumsum(onehot, axis=0)
    position = jnp.sum(onehot * running, axis=1) - 1
    target = pair_experts * capacity + position
    sources = jnp.arange(1, pair_experts.shape[0] + 1, dtype=jnp.int32)
    return jnp.zeros((EXPERTS * capacity,), jnp.int32).at[target].set(sources)


def newton_rows(rows_now, matrix, whole_now):
    left_product = jnp.einsum("eirk,eikc->eirc", rows_now, matrix, precision=lax.Precision.HIGHEST)
    return 2.0 * rows_now - jnp.einsum(
        "eirk,eikc->eirc", left_product, whole_now, precision=lax.Precision.HIGHEST
    )


def first_iterate(matrix, identity, inverse_bound):
    bound_scale = inverse_bound[:, :, None, None]
    return 2.0 * bound_scale * identity - bound_scale * bound_scale * matrix


def shared(features, gradients, route_ids, gate_share, token_mask, damping):
    tokens_here = features.shape[0]
    capacity = CAP
    blocks = 2 * NBLK
    kept_mask = token_mask.astype(jnp.float32)
    weight_pair = jnp.stack([gate_share, 1.0 - gate_share], axis=1) * kept_mask[:, None]
    kept_rows = features * token_mask.astype(jnp.bfloat16)[:, None]
    pair_grads = (gradients[:, None, :].astype(jnp.float32) * weight_pair[:, :, None]).astype(
        jnp.bfloat16
    )
    repeated = jnp.broadcast_to(kept_rows[:, None, :], pair_grads.shape)
    pair_rows = jnp.concatenate([repeated, pair_grads], axis=2).reshape(
        tokens_here * TOP, 2 * WIDTH
    )
    padded = jnp.concatenate([jnp.zeros((1, 2 * WIDTH), jnp.bfloat16), pair_rows], axis=0)
    buffer = jnp.take(padded, slot_table(route_ids, capacity), axis=0).reshape(
        EXPERTS, capacity, blocks, BLOCK
    )
    load_inverse = 1.0 / (
        tokens_here * lax.axis_size("expert") * lax.axis_size("dp") * TOP / EXPERTS
    )
    received = lax.all_to_all(buffer, "expert", split_axis=0, concat_axis=1, tiled=True)
    gram_blocks = (
        jnp.einsum("erib,eric->eibc", received, received, preferred_element_type=jnp.float32)
        * load_inverse
    )
    damping_flat = damping.reshape(damping.shape[0], blocks)[:, :, None, None]
    rows_share = BLOCK // lax.axis_size("dp")
    row_start = lax.axis_index("dp") * rows_share
    identity = jnp.eye(BLOCK, dtype=jnp.float32)
    summed = lax.psum(gram_blocks, "dp")
    matrix = summed + damping_flat * identity
    largest_sum = jnp.max(jnp.sum(jnp.abs(matrix), axis=3), axis=2)
    inverse_bound = 1.0 / largest_sum
    iterate_one = first_iterate(matrix, identity, inverse_bound)
    iterate_two = newton_rows(iterate_one, matrix, iterate_one)
    second_rows = lax.dynamic_slice_in_dim(iterate_two, row_start, rows_share, 2)
    third_rows = newton_rows(second_rows, matrix, iterate_two)
    act_rows = third_rows[:, :NBLK]
    grad_rows = third_rows[:, NBLK:]
    return (
        lax.all_gather(act_rows, "expert", axis=0, tiled=True),
        lax.all_gather(grad_rows, "expert", axis=0, tiled=True),
    )


def solution(mesh):
    placed = (
        P(("expert", "dp"), None),
        P(("expert", "dp"), None),
        P(("expert", "dp"), None),
        P(("expert", "dp")),
        P(("expert", "dp")),
        P("expert", None, None),
    )
    paired = mesh.shape["expert"] * mesh.shape["dp"] == 2 * MATRICES
    return jax.shard_map(
        owned if paired else shared,
        mesh=mesh,
        in_specs=placed,
        out_specs=(P(None, None, "dp", None), P(None, None, "dp", None)),
        check_vma=False,
    )
```

```python
import functools

import jax
import jax.numpy as jnp
from jax import lax
from jax.experimental import pallas as pl
from jax.experimental.pallas import tpu as pltpu
from jax.sharding import PartitionSpec as P


EXPERTS = 8
TOP = 2
BLOCK = 512
NBLK = 1
CAP = 64
WIDTH = 512
FACTORS = 2 * NBLK
MATRICES = EXPERTS * FACTORS
OWNERS = 2
LANES = 128
TILES = BLOCK // LANES
UPPER = [(top, left) for top in range(TILES) for left in range(top, TILES)]
VMEM_GRANT = 16 * 2**20
COLLECT_GRANT = 60 * 2**20
SENT_SCALE = 2.0**14
AXES = ("expert", "dp")


def whole(*shape):
    return pl.BlockSpec(memory_space=pltpu.VMEM)


META = 8
EARLY = (0, 7, 3, 6, 5)
LATE = (0, 1, 2, 4, 7, 3, 6, 5)


def chip_of(expert_shard, shard, shards):
    chips = shards // FACTORS // OWNERS
    return expert_shard * chips + lax.rem(shard, chips * OWNERS) // OWNERS


def collect_kernel(features, gradients, routes, share, mask, own, sent, ids, weight, kept, sems):
    tokens = features.shape[0]
    lower = lax.axis_index("dp") < lax.axis_size("dp") // FACTORS
    small = [
        pltpu.make_async_copy(routes, ids, sems.at[2]),
        pltpu.make_async_copy(share, weight, sems.at[3]),
        pltpu.make_async_copy(mask, kept, sems.at[4]),
    ]
    for copy in small:
        copy.start()

    def tokens_in(source, target, sem):
        return pltpu.make_async_copy(source, target.at[0:tokens], sems.at[sem])

    @pl.when(lower)
    def _():
        tokens_in(gradients, sent, 0).start()
        tokens_in(features, own, 1).start()

    @pl.when(jnp.logical_not(lower))
    def _():
        tokens_in(features, sent, 0).start()
        tokens_in(gradients, own, 1).start()

    for copy in small:
        copy.wait()
    high = weight[...].astype(jnp.bfloat16).astype(jnp.float32)
    rest = weight[...] - high
    middle = rest.astype(jnp.bfloat16).astype(jnp.float32)
    low = rest - middle
    first = jnp.concatenate(
        [
            ids[0:1, :].astype(jnp.float32),
            ids[1:2, :].astype(jnp.float32),
            kept[...].astype(jnp.float32),
            high,
        ],
        axis=1,
    )
    second = jnp.concatenate([middle, low, jnp.zeros_like(low), jnp.zeros_like(low)], axis=1)
    row = lax.broadcasted_iota(jnp.int32, (META, WIDTH), 0)
    meta = jnp.where(row == 0, first, jnp.where(row == 1, second, 0.0)).astype(jnp.bfloat16)
    own[tokens : tokens + META, :] = meta
    sent[tokens : tokens + META, :] = meta
    tokens_in(features, sent, 0).wait()
    tokens_in(features, own, 1).wait()


def pack_kernel(plan, *refs):
    inputs, outputs = refs[: len(plan)], refs[len(plan) :]
    tokens = inputs[0].shape[0] - META
    shard, shards = lax.axis_index("dp"), lax.axis_size("dp")
    lower = shard < shards // FACTORS
    chip = chip_of(lax.axis_index("expert"), shard, shards)
    expert = lax.broadcasted_iota(jnp.int32, (EXPERTS, tokens), 0)
    earlier = lax.broadcasted_iota(jnp.int32, (tokens, tokens), 0) < lax.broadcasted_iota(
        jnp.int32, (tokens, tokens), 1
    )
    earlier = jnp.where(earlier, 1.0, 0.0).astype(jnp.bfloat16)
    for package, places in zip(inputs, plan):
        slot = lax.broadcasted_iota(jnp.int32, (len(places) * CAP, tokens), 0)
        meta = package[tokens : tokens + META, :].astype(jnp.float32)

        def part(row, index):
            return meta[row : row + 1, index * tokens : (index + 1) * tokens]

        first = part(0, 0).astype(jnp.int32) ^ chip
        second = part(0, 1).astype(jnp.int32) ^ chip
        kept = part(0, 2)
        share = (part(0, 3) + part(1, 0)) + part(1, 1)
        is_first, is_second = expert == first, expert == second
        member = jnp.where(is_first | is_second, 1.0, 0.0).astype(jnp.bfloat16)
        position = jnp.dot(member, earlier, preferred_element_type=jnp.float32)
        wide = package[0:tokens, :].astype(jnp.float32)

        def picked(chosen, named):
            spot = jnp.sum(jnp.where(chosen, position, 0.0), axis=0, keepdims=True)
            base = jnp.full_like(named, -len(places) * CAP - CAP)
            for rank, (apart, _, _) in enumerate(places):
                base = jnp.where(named == apart, rank * CAP, base)
            hit = slot == base + spot.astype(jnp.int32)
            return jnp.where(hit, 1.0, 0.0).astype(jnp.bfloat16)

        def weighted(weight):
            weight = jnp.where(lower, kept, weight * kept)
            column = jnp.transpose(jnp.broadcast_to(weight, (tokens, tokens)))
            column = jnp.concatenate([column] * (WIDTH // tokens), axis=1)
            return (wide * column).astype(jnp.bfloat16)

        picks = jnp.concatenate([picked(is_first, first), picked(is_second, second)], axis=1)
        pairs = jnp.concatenate([weighted(share), weighted(1.0 - share)], axis=0)
        rows = jnp.dot(picks, pairs, preferred_element_type=jnp.float32).astype(jnp.bfloat16)
        for rank, (_, index, row) in enumerate(places):
            outputs[index][row : row + CAP, :] = rows[rank * CAP : (rank + 1) * CAP]


def gram_kernel(blocks, *refs):
    inputs, before, out = refs[:blocks], refs[blocks:-1], refs[-1]
    rows = jnp.concatenate([ref[...] for ref in inputs], axis=0)
    gram = lax.dot_general(
        rows, rows, (((0,), (0,)), ((), ())), preferred_element_type=jnp.float32
    )
    for index, (top, left) in enumerate(UPPER):
        tile = gram[top * LANES : (top + 1) * LANES, left * LANES : (left + 1) * LANES]
        for ref in before:
            tile = tile + ref[index]
        out[index] = tile


def split(value):
    high = value.astype(jnp.bfloat16)
    return high, (value - high.astype(jnp.float32)).astype(jnp.bfloat16)


def product(left, right):
    (left_high, left_low), (right_high, right_low) = left, right

    def dot(a, b):
        return jnp.dot(a, b, preferred_element_type=jnp.float32)

    return dot(left_high, right_high) + (dot(left_high, right_low) + dot(left_low, right_high))


def newton_kernel(load_inverse, owners, shards, damping, mine, other, out):
    shard = lax.axis_index("dp")
    core = lax.rem(shard, owners)
    factor = shard // (shards // FACTORS)
    expert = lax.rem(shard, shards // FACTORS) // owners
    place = lax.broadcasted_iota(jnp.int32, (BLOCK, BLOCK), 0)
    identity = jnp.where(place == lax.broadcasted_iota(jnp.int32, (BLOCK, BLOCK), 1), 1.0, 0.0)
    tiles = {}
    for index, (top, left) in enumerate(UPPER):
        tiles[top, left] = mine[index] + other[index]
        if top != left:
            tiles[left, top] = jnp.transpose(tiles[top, left])
    gram = jnp.concatenate(
        [
            jnp.concatenate([tiles[top, left] for left in range(TILES)], axis=1)
            for top in range(TILES)
        ],
        axis=0,
    )
    matrix = gram * load_inverse + damping[factor, expert] * identity
    bound = jnp.max(jnp.sum(jnp.abs(matrix), axis=0, keepdims=True), axis=1, keepdims=True)
    scale = 1.0 / bound
    error = identity - scale * matrix
    parts = split(error)
    cross = jnp.dot(parts[0], parts[1], preferred_element_type=jnp.float32)
    square = jnp.dot(parts[0], parts[0], preferred_element_type=jnp.float32)
    square = split(square + (cross + jnp.transpose(cross)))
    start = (identity + error).reshape(shards // owners, owners, BLOCK // shards, BLOCK)
    rows = start[:, 0]
    for turn in range(1, owners):
        rows = jnp.where(core == turn, start[:, turn], rows)
    rows = rows.reshape(BLOCK // owners, BLOCK)
    rows = rows + product(split(rows), square)
    last = rows + product(split(product(split(rows), square)), square)
    last = (scale * SENT_SCALE) * last
    encode(core, shards, owners, last, out)


def encode(core, shards, owners, rows, out):
    share = BLOCK // shards
    out[...] = rows
    turns = shards // owners
    starts = [turn * owners * share // LANES * LANES for turn in range(turns)]
    tile = jnp.concatenate(
        [
            rows[turn * share : (turn + 1) * share, start : start + LANES]
            for turn, start in enumerate(starts)
        ],
        axis=0,
    )
    place = lax.broadcasted_iota(jnp.int32, tile.shape, 0)
    row = lax.rem(place, share)
    first = lax.rem(place // share * (owners * share), LANES) + core * share
    column = lax.broadcasted_iota(jnp.int32, tile.shape, 1) - first
    high = tile.astype(jnp.bfloat16).astype(jnp.float32)
    low = tile - high
    beside = pltpu.roll(low, LANES - 1, 1)
    tile = jnp.where(column == row, high, tile)
    tile = jnp.where((column == row - 1) & (row > 0), beside, tile)
    tile = jnp.where((column == 0) & (row == 2), pltpu.roll(low, 2, 0), tile)
    for turn, start in enumerate(starts):
        part = slice(turn * share, (turn + 1) * share)
        out[part, start : start + LANES] = tile[part]


def decode_kernel(rows, act, grad, results, sems):
    groups, share = lax.axis_size("expert"), act.shape[2]
    first = lax.axis_index("dp") * share
    start = pl.multiple_of(first // LANES * LANES, LANES)
    total = rows.shape[0]
    tile = rows[:, pl.ds(start, LANES)]
    row = lax.rem(lax.broadcasted_iota(jnp.int32, (total, LANES), 0), share)
    column = lax.broadcasted_iota(jnp.int32, (total, LANES), 1) - (first - start)

    def moved(down, right):
        value = tile
        if down:
            value = pltpu.roll(value, down % total, 0)
        if right:
            value = pltpu.roll(value, right % LANES, 1)
        return value

    fixed = jnp.where(column == row, tile + jnp.where(row > 0, moved(0, 1), moved(-2, 0)), tile)
    fixed = jnp.where((column == row - 1) & (row > 0), moved(1, -1), fixed)
    fixed = jnp.where((column == 0) & (row == 2), moved(2, -2), fixed)

    def of_factor(value, factor):
        value = value.reshape(groups, FACTORS, EXPERTS // groups, share, value.shape[-1])
        return value[:, factor].reshape(EXPERTS, share, value.shape[-1])

    copies = []
    for factor, out in ((0, act), (1, grad)):
        results[factor] = of_factor(rows[...], factor)
        results[factor, :, :, pl.ds(start, LANES)] = of_factor(fixed, factor)
        copies.append(pltpu.make_async_copy(results.at[factor], out.at[:, 0], sems.at[factor]))
        copies[-1].start()
    for copy in copies:
        copy.wait()


def owned(features, gradients, route_ids, gate_share, token_mask, damping):
    tokens = features.shape[0]
    experts_axis, shards = lax.axis_size("expert"), lax.axis_size("dp")
    devices = experts_axis * shards
    owners = devices // MATRICES
    load_inverse = 1.0 / (tokens * devices * TOP / EXPERTS)
    spec = whole()
    params = pltpu.CompilerParams(vmem_limit_bytes=VMEM_GRANT)
    package = pltpu.VMEM((tokens + META, WIDTH), jnp.bfloat16)
    own, sent = pl.pallas_call(
        collect_kernel,
        out_shape=(package, package),
        in_specs=[pl.BlockSpec(memory_space=pltpu.HBM)] * 5,
        out_specs=(spec, spec),
        scratch_shapes=[
            pltpu.VMEM((TOP, tokens), jnp.int32),
            pltpu.VMEM((1, tokens), jnp.float32),
            pltpu.VMEM((1, tokens), jnp.int32),
            pltpu.SemaphoreType.DMA((5,)),
        ],
        compiler_params=pltpu.CompilerParams(vmem_limit_bytes=COLLECT_GRANT),
        name="collect",
    )(
        features,
        gradients,
        route_ids.T,
        gate_share.reshape(1, tokens),
        token_mask.reshape(1, tokens),
    )
    far = shards // FACTORS
    chips = far // owners

    def pack(packages, wanted):
        plan, sizes = [[] for _ in packages], []
        for index, (apart, sources) in enumerate(wanted):
            for order, source in enumerate(sources):
                plan[source].append((apart, index, order * CAP))
            sizes.append(len(sources) * CAP)
        return pl.pallas_call(
            functools.partial(pack_kernel, plan),
            out_shape=[pltpu.VMEM((size, WIDTH), jnp.bfloat16) for size in sizes],
            in_specs=[spec] * len(packages),
            out_specs=[spec] * len(sizes),
            compiler_params=params,
            name="pack",
        )(*packages)

    def deliver(block, step):
        if step == 0:
            return block
        apart = step // chips * shards + step % chips * owners
        return lax.ppermute(block, AXES, [(i, i ^ apart) for i in range(devices)])

    early = [(step, (0,)) for step in EARLY]
    late = [(step, (1,) if step in EARLY else (0, 1)) for step in LATE]
    got = lax.ppermute(sent, "dp", [(i, (i + far) % shards) for i in range(shards)])
    blocks = pack([own], early)
    received = []
    for block, (step, _) in zip(blocks, early):
        received.append(deliver(block, step))
    blocks = pack([own, got], late)
    last = []
    for block, (step, _) in zip(blocks, late):
        (last if step in EARLY[1:] else received).append(deliver(block, step))

    def gram(blocks, *before):
        return pl.pallas_call(
            functools.partial(gram_kernel, len(blocks)),
            out_shape=pltpu.VMEM((len(UPPER), LANES, LANES), jnp.float32),
            in_specs=[spec] * (len(blocks) + len(before)),
            out_specs=spec,
            compiler_params=params,
            name="gram",
        )(*blocks, *before)

    partial = gram(received)
    mine = gram(last, partial)
    other = lax.ppermute(mine, "dp", [(i, i ^ 1) for i in range(shards)])
    rows = pl.pallas_call(
        functools.partial(newton_kernel, load_inverse, owners, shards),
        out_shape=pltpu.VMEM((BLOCK // owners, BLOCK), jnp.float32),
        in_specs=[pl.BlockSpec(memory_space=pltpu.SMEM), spec, spec],
        out_specs=spec,
        compiler_params=params,
        name="newton",
    )(damping.reshape(-1, FACTORS).T, mine, other)
    sent = jnp.concatenate([rows.astype(jnp.float16)] * experts_axis, axis=0)
    lanes = range(owners)
    same_core = [
        [e * shards + i + c for e in range(experts_axis) for i in range(0, shards, owners)]
        for c in lanes
    ]
    gathered = lax.all_to_all(
        sent, AXES, split_axis=0, concat_axis=0, tiled=True, axis_index_groups=same_core
    )
    result = jax.ShapeDtypeStruct((EXPERTS, NBLK, BLOCK // shards, BLOCK), jnp.float32)
    return pl.pallas_call(
        decode_kernel,
        out_shape=(result, result),
        in_specs=[spec],
        out_specs=(pl.BlockSpec(memory_space=pltpu.HBM),) * FACTORS,
        scratch_shapes=[
            pltpu.VMEM((FACTORS, EXPERTS, BLOCK // shards, BLOCK), jnp.float32),
            pltpu.SemaphoreType.DMA((FACTORS,)),
        ],
        compiler_params=params,
        name="decode",
    )(gathered.astype(jnp.float32) * (1.0 / SENT_SCALE))


def slot_table(route_ids, capacity):
    pair_experts = route_ids.reshape(-1)
    onehot = (pair_experts[:, None] == jnp.arange(EXPERTS, dtype=jnp.int32)[None, :]).astype(
        jnp.int32
    )
    running = jnp.cumsum(onehot, axis=0)
    position = jnp.sum(onehot * running, axis=1) - 1
    target = pair_experts * capacity + position
    sources = jnp.arange(1, pair_experts.shape[0] + 1, dtype=jnp.int32)
    return jnp.zeros((EXPERTS * capacity,), jnp.int32).at[target].set(sources)


def newton_rows(rows_now, matrix, whole_now):
    left_product = jnp.einsum("eirk,eikc->eirc", rows_now, matrix, precision=lax.Precision.HIGHEST)
    return 2.0 * rows_now - jnp.einsum(
        "eirk,eikc->eirc", left_product, whole_now, precision=lax.Precision.HIGHEST
    )


def first_iterate(matrix, identity, inverse_bound):
    bound_scale = inverse_bound[:, :, None, None]
    return 2.0 * bound_scale * identity - bound_scale * bound_scale * matrix


def shared(features, gradients, route_ids, gate_share, token_mask, damping):
    tokens_here = features.shape[0]
    capacity = CAP
    blocks = 2 * NBLK
    kept_mask = token_mask.astype(jnp.float32)
    weight_pair = jnp.stack([gate_share, 1.0 - gate_share], axis=1) * kept_mask[:, None]
    kept_rows = features * token_mask.astype(jnp.bfloat16)[:, None]
    pair_grads = (gradients[:, None, :].astype(jnp.float32) * weight_pair[:, :, None]).astype(
        jnp.bfloat16
    )
    repeated = jnp.broadcast_to(kept_rows[:, None, :], pair_grads.shape)
    pair_rows = jnp.concatenate([repeated, pair_grads], axis=2).reshape(
        tokens_here * TOP, 2 * WIDTH
    )
    padded = jnp.concatenate([jnp.zeros((1, 2 * WIDTH), jnp.bfloat16), pair_rows], axis=0)
    buffer = jnp.take(padded, slot_table(route_ids, capacity), axis=0).reshape(
        EXPERTS, capacity, blocks, BLOCK
    )
    load_inverse = 1.0 / (
        tokens_here * lax.axis_size("expert") * lax.axis_size("dp") * TOP / EXPERTS
    )
    received = lax.all_to_all(buffer, "expert", split_axis=0, concat_axis=1, tiled=True)
    gram_blocks = (
        jnp.einsum("erib,eric->eibc", received, received, preferred_element_type=jnp.float32)
        * load_inverse
    )
    damping_flat = damping.reshape(damping.shape[0], blocks)[:, :, None, None]
    rows_share = BLOCK // lax.axis_size("dp")
    row_start = lax.axis_index("dp") * rows_share
    identity = jnp.eye(BLOCK, dtype=jnp.float32)
    summed = lax.psum(gram_blocks, "dp")
    matrix = summed + damping_flat * identity
    largest_sum = jnp.max(jnp.sum(jnp.abs(matrix), axis=3), axis=2)
    inverse_bound = 1.0 / largest_sum
    iterate_one = first_iterate(matrix, identity, inverse_bound)
    iterate_two = newton_rows(iterate_one, matrix, iterate_one)
    second_rows = lax.dynamic_slice_in_dim(iterate_two, row_start, rows_share, 2)
    third_rows = newton_rows(second_rows, matrix, iterate_two)
    act_rows = third_rows[:, :NBLK]
    grad_rows = third_rows[:, NBLK:]
    return (
        lax.all_gather(act_rows, "expert", axis=0, tiled=True),
        lax.all_gather(grad_rows, "expert", axis=0, tiled=True),
    )


def solution(mesh):
    placed = (
        P(("expert", "dp"), None),
        P(("expert", "dp"), None),
        P(("expert", "dp"), None),
        P(("expert", "dp")),
        P(("expert", "dp")),
        P("expert", None, None),
    )
    paired = mesh.shape["expert"] * mesh.shape["dp"] == 2 * MATRICES
    return jax.shard_map(
        owned if paired else shared,
        mesh=mesh,
        in_specs=placed,
        out_specs=(P(None, None, "dp", None), P(None, None, "dp", None)),
        check_vma=False,
    )
```
